512 devices in a mesh: dp: 64 (over z, x), vocab: 8 (over y, core).
Axes of the slice: x: 4, y: 4, z: 16, core: 2. Of those that a mesh axis runs over, the one named last changes fastest.
Arguments:
- tokens: int32 [576, 512], P('dp'), may hold values from 0 to 32127
- span_bounds: int32 [576, 16, 2], P('dp'), may hold values from 1 to 512, as said below
- owner: int32 [576, 80, 1], P('dp'), may hold values from 0 to 63; in each aligned block of 720 rows (0 to 719, 720 to 1439, ..., all dimensions but the last counted through in order) at most 12 rows name the same one
- decoder_states: bfloat16 [576, 80, 1024], P('dp', None, 'vocab'), may hold values from -1024 to 1024
- norm_gain: bfloat16 [1024], replicated, may hold values from 0.25 to 1.75
- embedding: bfloat16 [32128, 1024], P('vocab', 'dp'), may hold values from -64 to 64
Outputs:
- losses: float32 [49152], P('dp')
The draws below stay inside these ranges and needn't reach their ends.
Inputs may be any that keep to these rules, and one draw needn't show every extreme that they name: `span_bounds`: within a sequence the 16 spans are disjoint and in increasing order, each with span_end - span_start from 1 to 5; every sequence has a span of exactly 5. Among the slots of one dp device no owner is named more than 12 times; in some of those blocks an owner is named exactly 12 times.
All inputs are finite; a program needn't handle non-finite values.
Results may differ from the reference program's by a relative error of at most 0.00047.
Values may be sent and summed in bfloat16 or wider, within the bound.
No kernel may reach another device: no remote copies, remote signals or barrier semaphores. Data moves between devices by JAX's collectives and lax.ppermute only.
A program may use at most 64 MiB of HBM per device.

```python
import math
import jax
import jax.numpy as jnp
import numpy as np
from jax import lax

D = 1024
VOCAB = 32128
LEN = 512
NSPAN = 16
MAXSPAN = 5
SEQ_DEV = 9
SEQS = 576
OWN_ROWS = 768
CAP = 12
N_DP = 64


def draw_span_bounds(key, part):
    key_len, key_long, key_gap = jax.random.split(jax.random.fold_in(key, 11), 3)
    lengths = jax.random.randint(key_len, (SEQS, NSPAN), 1, MAXSPAN + 1)
    longest = jax.random.randint(key_long, (SEQS, 1), 0, NSPAN)
    lengths = jnp.where(jnp.arange(NSPAN)[None, :] == longest, MAXSPAN, lengths)
    spacing = jax.random.randint(key_gap, (SEQS, NSPAN), 1, LEN // NSPAN - MAXSPAN + 1)
    span_ends = jnp.cumsum(spacing + lengths, axis=1)
    shifted = span_ends + (LEN - span_ends[:, -1:])
    starts = shifted - lengths
    return jnp.stack([starts, shifted], axis=-1).astype(jnp.int32)


def shared_patterns(key):
    key_col, key_topic, key_lead = jax.random.split(jax.random.fold_in(key, 7), 3)
    topic_count = max(4, min(32, VOCAB // 1000))
    col_scale = jnp.exp(jax.random.uniform(key_col, (D,), jnp.float32, math.log(0.5), math.log(2.0)))
    col_scale = col_scale / jnp.sqrt(jnp.mean(col_scale * col_scale))
    raw = jax.random.normal(key_topic, (topic_count, D), jnp.float32) / col_scale[None, :]
    topics = raw / jnp.sqrt(jnp.sum(raw * raw, axis=1, keepdims=True))
    pattern = 102.4 / math.sqrt(D) * jnp.clip(jax.random.normal(key_lead, (8, D), jnp.float32), -1.4, 1.4)
    leading = pattern * jnp.linspace(1.4, 3.8, 8).astype(jnp.float32)[:, None]
    return (col_scale, topics, leading)


def draw_embedding(key, part):
    col_scale, topics, leading = shared_patterns(key)
    key_perm, key_base, key_row, key_strength, key_noise = jax.random.split(jax.random.fold_in(key, 31), 5)
    topic_count = topics.shape[0]
    heavy_count = max(4, VOCAB // 64)
    order = jax.random.permutation(key_perm, VOCAB)
    leading_rows = order[:8]
    runner_rows = order[8:16]
    topic_rows = order[16:16 + heavy_count]
    row_scale = jnp.exp(jax.random.uniform(key_row, (VOCAB, 1), jnp.float32, 0.0, math.log(4.0)))
    vocab_table = 1.5 * jnp.clip(jax.random.normal(key_base, (VOCAB, D), jnp.float32), -4.0, 4.0) * row_scale * col_scale[None, :]
    strength = jax.random.uniform(key_strength, (heavy_count, 1), jnp.float32, 2.0, 3.2) * math.log(VOCAB)
    topic_ids = jnp.arange(heavy_count) % topic_count
    vocab_table = vocab_table.at[topic_rows].add(strength * topics[topic_ids])
    length = jnp.sqrt(jnp.sum(leading * leading, axis=1, keepdims=True))
    runner = jnp.clip(leading - 2.0 * leading / length + 0.3 * jax.random.normal(key_noise, (8, D), jnp.float32), -64.0, 64.0)
    vocab_table = vocab_table.at[leading_rows].set(leading).at[runner_rows].set(runner)
    return jnp.clip(vocab_table, -64.0, 64.0).astype(jnp.bfloat16)


def draw_decoder_states(key, part):
    col_scale, topics, leading = shared_patterns(key)
    key_row = jax.random.fold_in(jax.random.fold_in(key, 23), 0)
    key_col = jax.random.fold_in(jax.random.fold_in(key, 23), 1)
    key_body = jax.random.fold_in(jax.random.fold_in(key, 23), 3)
    key_pick = jax.random.fold_in(jax.random.fold_in(key, 23), 4)
    key_which = jax.random.fold_in(jax.random.fold_in(key, 23), 5)
    key_topic = jax.random.fold_in(jax.random.fold_in(key, 23), 6)
    key_cos = jax.random.fold_in(jax.random.fold_in(key, 23), 7)
    slot_count = NSPAN * MAXSPAN
    shape = (SEQS, slot_count, D)
    row_scale = jnp.exp(jax.random.uniform(key_row, (SEQS, slot_count, 1), jnp.float32, 0.0, math.log(10.0)))
    state_cols = jnp.exp(jax.random.uniform(key_col, (D,), jnp.float32, 0.0, math.log(10.0)))
    noise = jnp.clip(jax.random.normal(key_body, shape, jnp.float32), -4.0, 4.0) * state_cols
    noise = noise / jnp.sqrt(jnp.sum(noise * noise, axis=2, keepdims=True))
    topic_pick = jax.random.randint(key_topic, (SEQS, slot_count), 0, topics.shape[0])
    cosine = jax.random.uniform(key_cos, (SEQS, slot_count, 1), jnp.float32, 0.5, 0.85)
    direction = cosine * topics[topic_pick] + jnp.sqrt(1.0 - cosine * cosine) * noise
    states = direction * math.sqrt(D) * row_scale
    forced = (jnp.arange(SEQS)[:, None] == 0) & (jnp.arange(slot_count)[None, :] == 0)
    picked = jax.random.bernoulli(key_pick, 0.005, (SEQS, slot_count)) | forced
    which = jax.random.randint(key_which, (SEQS, slot_count), 0, 8)
    aligned = leading[which] * row_scale * 0.25
    states = jnp.where(picked[:, :, None], aligned, states)
    return jnp.clip(states, -1024.0, 1024.0).astype(jnp.bfloat16)


def touch_ends(values, key, smallest, high):
    longest = values.shape.index(max(values.shape))
    spots = []
    for shift in (0, 1):
        where = [jax.random.randint(jax.random.fold_in(key, axis), (), 0, length) for axis, length in enumerate(values.shape)]
        where[longest] = (where[longest] + shift) % values.shape[longest]
        spots.append(tuple(where))
    return values.at[spots[0]].set(smallest).at[spots[1]].set(high)


def rank_table(count, lean):
    weights = [(1 << 20) // math.isqrt(grade ** lean) + 1 for grade in range(1, count + 1)]
    scale = 1 + sum(weights) // (1 << 30)
    return np.cumsum(np.array([max(1, weight // scale) for weight in weights]))


def ranked(stream_key, extent, amount, slope):
    listing = rank_table(amount, slope)
    ticket = jax.random.randint(jax.random.fold_in(stream_key, 1), extent, 0, int(listing[amount - 1]))
    standing = jnp.searchsorted(jnp.asarray(listing, jnp.int32), ticket, side="right")
    return jax.random.permutation(jax.random.fold_in(stream_key, 2), amount)[standing].astype(jnp.int32)


def routed_block(key, own, number, rows, amount, top, reach, lean):
    ranking = jax.random.permutation(key, amount)
    heavy_load, usual = portions_of(amount, rows * top, reach, lean, True), portions_of(amount, rows * top, reach, lean, False)
    places = jnp.arange(amount)

    def named(sizes, rotation):
        used = int((sizes > 0).sum())
        fixed = max(1, used // 4)
        passed = fixed + (places - fixed + rotation * (used - fixed)) % max(1, amount - fixed)
        return jnp.zeros((amount,), jnp.int32).at[ranking[jnp.where(places < fixed, places, passed)]].set(jnp.asarray(sizes, jnp.int32))

    sizes = jnp.where(number % 4 == 0, named(heavy_load, number // 4), named(usual, number - number // 4 - 1))
    mixed = jax.random.permutation(jax.random.fold_in(own, 3), amount)
    donor, receiver = mixed[0:amount // 2 * 2:2], mixed[1:amount // 2 * 2:2]
    room = jnp.minimum(sizes[donor] - 1, reach - sizes[receiver]) // 2
    room = jnp.where((donor == ranking[0]) | (receiver == ranking[0]) | (sizes[receiver] == 0), 0, jnp.maximum(room, 0))
    passed = jax.random.randint(jax.random.fold_in(own, 4), (amount // 2,), 0, 1 << 20) % (room + 1)
    sizes = sizes.at[donor].add(-passed).at[receiver].add(passed)
    items = jnp.searchsorted(jnp.cumsum(sizes), jnp.arange(rows * top), side="right").astype(jnp.int32)
    grid = items.reshape(top, rows).T
    grid = grid[jax.random.permutation(jax.random.fold_in(own, 1), rows)]
    rotation = jax.random.randint(jax.random.fold_in(own, 2), (rows, 1), 0, top)
    return jnp.take_along_axis(grid, (jnp.arange(top)[None, :] + rotation) % top, axis=1)


def portions_of(count, total, most, slope, full):
    loads = [(1 << 20) // math.isqrt(rank ** slope) + 1 for rank in range(1, count + 1)]
    largest = most if full else min(most, max(-(-total // count), total * loads[0] // sum(loads)))
    least = 1 if total - largest >= count - 1 else 0
    counts, surplus = [largest] + [least] * (count - 1), total - largest - least * (count - 1)
    while surplus > 0:
        movable = [i for i in range(1, count) if counts[i] < largest] or [i for i in range(1, count) if counts[i] < most]
        whole, left = sum([loads[i] for i in movable]), surplus
        for i in movable:
            extra = min(most - counts[i], max(1, left * loads[i] // whole), surplus)
            counts[i] = counts[i] + extra
            surplus = surplus - extra
    return np.array(counts)


def setup_inputs(seed: int = 0) -> dict:
    streams_of = jax.random.split(jax.random.key(seed), 7)
    tokens = touch_ends(ranked(streams_of[0], (SEQS, LEN), VOCAB, 2), jax.random.fold_in(streams_of[0], 3), 0, VOCAB - 1).astype(jnp.int32)
    span_bounds = draw_span_bounds(jax.random.fold_in(streams_of[6], 71), 0)
    owner_keys = jax.random.split(jax.random.fold_in(streams_of[2], 1), SEQS * (NSPAN * MAXSPAN) // (SEQ_DEV * NSPAN * MAXSPAN))
    owner_turns = jax.random.permutation(jax.random.fold_in(streams_of[2], 3), SEQS * (NSPAN * MAXSPAN) // (SEQ_DEV * NSPAN * MAXSPAN))
    owner = jax.vmap(lambda own, number: routed_block(jax.random.fold_in(streams_of[2], 2), own, number, SEQ_DEV * NSPAN * MAXSPAN, N_DP, 1, CAP, 2))(owner_keys, owner_turns).reshape((SEQS, NSPAN * MAXSPAN, 1))
    decoder_states = draw_decoder_states(jax.random.fold_in(streams_of[6], 71), 0)
    norm_gain = jnp.clip(1.0 + 0.15 * jax.random.normal(streams_of[4], (D,), jnp.float32), 0.25, 1.75).astype(jnp.bfloat16)
    embedding = draw_embedding(jax.random.fold_in(streams_of[6], 71), 0)
    return dict(tokens=tokens, span_bounds=span_bounds, owner=owner, decoder_states=decoder_states, norm_gain=norm_gain, embedding=embedding)


epsilon = 1e-06

def reference(tokens, span_bounds, owner, decoder_states, norm_gain, embedding):
    slot_count = NSPAN * MAXSPAN
    slot_ids = jnp.arange(slot_count, dtype=jnp.int32)
    offsets = slot_ids % MAXSPAN
    starts = jnp.repeat(span_bounds[:, :, 0], MAXSPAN, axis=1)
    span_ends = jnp.repeat(span_bounds[:, :, 1], MAXSPAN, axis=1)
    is_live = offsets[None, :] < span_ends - starts
    positions = jnp.minimum(starts + offsets[None, :], LEN - 1).astype(jnp.int32)
    labels = jnp.take_along_axis(tokens, positions, axis=1)
    device_slots = SEQ_DEV * slot_count
    targets = owner.reshape(N_DP, device_slots)
    owner_hits = (targets[:, :, None] == jnp.arange(N_DP, dtype=jnp.int32)[None, None, :]).astype(jnp.int32)
    running = jnp.cumsum(owner_hits, axis=1) - owner_hits
    slot_rank = lax.optimization_barrier(jnp.sum(running * owner_hits, axis=2)).astype(jnp.int32)
    source = jnp.arange(N_DP, dtype=jnp.int32)[:, None]
    target_row = (targets * OWN_ROWS + source * CAP + slot_rank).astype(jnp.int32)
    states = decoder_states.reshape(N_DP, device_slots, D).astype(jnp.float32)
    mean_square = lax.optimization_barrier(jnp.mean(states * states, axis=2, keepdims=True))
    normed = (states * lax.rsqrt(mean_square + epsilon) * norm_gain.astype(jnp.float32) * D ** (-0.5)).astype(jnp.bfloat16)

    def device_loss(operands):
        row_block, row_labels = operands
        logits = lax.dot_general(row_block, embedding, (((1,), (1,)), ((), ())), preferred_element_type=jnp.float32)
        row_top = lax.optimization_barrier(jnp.max(logits, axis=1))
        exp_total = lax.optimization_barrier(jnp.sum(jnp.exp(logits - row_top[:, None]), axis=1))
        label_logit = jnp.take_along_axis(logits, row_labels[:, None].astype(jnp.int32), axis=1)[:, 0]
        return row_top + jnp.log(exp_total) - label_logit
    row_loss = lax.map(device_loss, (normed, labels.reshape(N_DP, device_slots)))
    live_flat = is_live.reshape(-1)
    slot_index = jnp.where(live_flat, target_row.reshape(-1), N_DP * OWN_ROWS).astype(jnp.int32)
    result = jnp.zeros((N_DP * OWN_ROWS,), jnp.float32)
    return result.at[slot_index].set(jnp.where(live_flat, row_loss.reshape(-1), 0.0).astype(jnp.float32), mode='drop')
```

```python
import jax
import jax.numpy as jnp
from jax import lax
from jax.experimental import pallas as pl
from jax.experimental.pallas import tpu as pltpu
from jax.sharding import Mesh
from jax.sharding import PartitionSpec as P

MAXSPAN = 5
OWN_ROWS = 768
DP = ("z", "x")
VOC = ("y", "c")
PLANE = ("x", "y", "c")

epsilon = 1e-06


ROW_BLOCK = 256
MATMUL_ROWS = 512
LANES = 128


def broadcast_all(value, axis):
    copies = jnp.broadcast_to(value, (lax.axis_size(axis), *value.shape))
    return lax.all_to_all(copies, axis, split_axis=0, concat_axis=0, tiled=True)


def swap_cores(value):
    return lax.ppermute(value, "c", [(0, 1), (1, 0)])


def part_width(rows, parts):
    return -(-rows // (parts * LANES)) * LANES


def exchanged_embedding(embedding):
    parts = lax.axis_size("x")
    local = embedding.T
    width, rows = local.shape
    part = part_width(rows, parts)
    local = jnp.pad(local, ((0, 0), (0, part * parts - rows)))
    split = jnp.stack([local[:, k * part : (k + 1) * part] for k in range(parts)])
    mixed = lax.all_to_all(split, "x", split_axis=0, concat_axis=0, tiled=True)
    return mixed.reshape(parts * width, part)


def packed_rows(tokens, span_bounds, owner, decoder_states):
    seq_count, slot_count, local_width = decoder_states.shape
    planes, columns = lax.axis_size("z"), lax.axis_size("x")
    owner_total = planes * columns
    capacity = OWN_ROWS // owner_total
    slot_ids = jnp.arange(slot_count, dtype=jnp.int32)
    offsets = slot_ids % MAXSPAN
    starts = jnp.repeat(span_bounds[:, :, 0], MAXSPAN, axis=1)
    span_ends = jnp.repeat(span_bounds[:, :, 1], MAXSPAN, axis=1)
    is_live = (offsets[None, :] < span_ends - starts).reshape(-1)
    length = tokens.shape[1]
    positions = jnp.minimum(starts + offsets[None, :], length - 1)
    places = jnp.arange(length, dtype=jnp.int32)
    labels = jnp.sum(
        jnp.where(places[None, None, :] == positions[:, :, None], tokens[:, None, :], 0), axis=2
    ).reshape(-1)
    targets = owner.reshape(-1)
    slot_total = targets.shape[0]
    owner_hits = (targets[:, None] == jnp.arange(owner_total, dtype=jnp.int32)[None, :]).astype(
        jnp.bfloat16
    )
    device_slots = jnp.arange(slot_total, dtype=jnp.int32)
    earlier = (device_slots[:, None] > device_slots[None, :]).astype(jnp.bfloat16)
    running = jnp.dot(earlier, owner_hits, preferred_element_type=jnp.float32)
    slot_rank = jnp.sum(running * owner_hits.astype(jnp.float32), axis=1).astype(jnp.int32)
    place = (targets % columns) * planes + targets // columns
    target_row = place * capacity + slot_rank
    placing = (target_row[None, :] == jnp.arange(OWN_ROWS, dtype=jnp.int32)[:, None]) & is_live[
        None, :
    ]
    sent_labels = jnp.sum(jnp.where(placing, labels[None, :] + 1, 0), axis=1)
    onehot = placing.astype(jnp.bfloat16)
    states = decoder_states.reshape(slot_total, local_width)
    packed = jnp.dot(onehot, states, preferred_element_type=jnp.float32).astype(jnp.bfloat16)
    return packed, sent_labels


def normalize_block(core_ref, near_ref, far_ref, gain_ref, out_ref):
    first = core_ref[0] == 0
    pieces = []
    for k in range(near_ref.shape[1]):
        near = near_ref[0, k].astype(jnp.float32)
        far = far_ref[0, k].astype(jnp.float32)
        pieces += [jnp.where(first, near, far), jnp.where(first, far, near)]
    squares = pieces[0] * pieces[0]
    for piece in pieces[1:]:
        squares = squares + piece * piece
    width = len(pieces) * LANES
    mean_square = jnp.sum(squares, axis=1, keepdims=True) / width
    scale = lax.rsqrt(mean_square + epsilon)
    for k, piece in enumerate(pieces):
        gain = gain_ref[0:1, k * LANES : (k + 1) * LANES]
        out_ref[:, k * LANES : (k + 1) * LANES] = (
            piece * scale * gain * width ** (-0.5)
        ).astype(jnp.bfloat16)


def normalized(near, far, norm_gain):
    columns, slices = near.shape[:2]
    blocks = OWN_ROWS // ROW_BLOCK
    width = slices * 2 * LANES
    core = lax.axis_index("c").reshape(1)
    gain = norm_gain.astype(jnp.float32).reshape(1, width)
    spec = pl.BlockSpec((1, slices, ROW_BLOCK, LANES), lambda x, i, core: (x, 0, i, 0))
    return pl.pallas_call(
        normalize_block,
        grid_spec=pltpu.PrefetchScalarGridSpec(
            num_scalar_prefetch=1,
            grid=(columns, blocks),
            in_specs=[spec, spec, pl.BlockSpec((1, width), lambda x, i, core: (0, 0))],
            out_specs=pl.BlockSpec((ROW_BLOCK, width), lambda x, i, core: (x * blocks + i, 0)),
        ),
        out_shape=jax.ShapeDtypeStruct((columns * OWN_ROWS, width), jnp.bfloat16),
        name="normalized",
    )(core, near, far, gain)


def stats_block(valid_ref, rows_ref, weights_ref, labels_ref, out_ref):
    rows = rows_ref.shape[0]
    logits = jnp.dot(rows_ref[...], weights_ref[...], preferred_element_type=jnp.float32)
    columns = lax.broadcasted_iota(jnp.int32, logits.shape, 1)
    logits = jnp.where(columns < valid_ref[0], logits, -jnp.inf)
    top = jnp.max(logits, axis=1, keepdims=True)
    total = jnp.sum(jnp.exp(logits - top), axis=1, keepdims=True)
    label = jnp.broadcast_to(labels_ref[0:1, :], (LANES, rows)).T[:, 0:1]
    picked = jnp.sum(jnp.where(columns == label, logits, 0.0), axis=1, keepdims=True)
    lane = lax.broadcasted_iota(jnp.int32, (rows, LANES), 1)
    both = jnp.where(lane == 0, top + jnp.log(total), picked)
    out_ref[...] = both.T[0:8]


def row_stats(rows, weights, labels, valid):
    total, width = rows.shape
    part = weights.shape[1]
    stats = pl.pallas_call(
        stats_block,
        grid_spec=pltpu.PrefetchScalarGridSpec(
            num_scalar_prefetch=1,
            grid=(total // MATMUL_ROWS,),
            in_specs=[
                pl.BlockSpec((MATMUL_ROWS, width), lambda i, valid: (i, 0)),
                pl.BlockSpec((width, part), lambda i, valid: (0, 0)),
                pl.BlockSpec((1, MATMUL_ROWS), lambda i, valid: (0, i)),
            ],
            out_specs=pl.BlockSpec((8, MATMUL_ROWS), lambda i, valid: (0, i)),
        ),
        out_shape=jax.ShapeDtypeStruct((8, total), jnp.float32),
        name="row_stats",
    )(valid.reshape(1), rows, weights, labels.reshape(1, total))
    return stats[:2]


def on_device(tokens, span_bounds, owner, decoder_states, norm_gain, embedding):
    planes, columns = lax.axis_size("z"), lax.axis_size("x")
    capacity = OWN_ROWS // (planes * columns)
    shard_rows = embedding.shape[0]
    mixed = exchanged_embedding(embedding)
    mixed, tokens, span_bounds, owner, decoder_states = lax.optimization_barrier(
        (mixed, tokens, span_bounds, owner, decoder_states)
    )
    weights = lax.all_gather(mixed, "z", axis=0, tiled=True)
    packed, sent_labels = packed_rows(tokens, span_bounds, owner, decoder_states)
    digits = jnp.stack([sent_labels // 256, sent_labels % 256]).astype(jnp.bfloat16)
    digits = digits.reshape(-1, LANES)
    digits = jnp.pad(digits, ((0, -digits.shape[0] % 16), (0, 0)))
    bundle = jnp.concatenate([packed, digits], axis=0)
    near = broadcast_all(bundle, ("x", "y"))
    far = swap_cores(near)
    near = near.reshape(columns, -1, *bundle.shape)
    far = far.reshape(near.shape)
    tags = near[:, 0, OWN_ROWS : OWN_ROWS + 2 * OWN_ROWS // LANES].astype(jnp.int32)
    tags = tags.reshape(columns, 2, OWN_ROWS)
    row_labels = tags[:, 0] * 256 + tags[:, 1] - 1
    part = mixed.shape[1]
    here = lax.axis_index("x")
    valid = jnp.minimum(shard_rows - here * part, part)
    local_label = row_labels - (lax.axis_index(VOC) * shard_rows + here * part)
    local_label = jnp.where((local_label >= 0) & (local_label < valid), local_label, -1)
    rows = normalized(near, far, norm_gain)
    stats = row_stats(rows, weights, local_label.reshape(-1), valid)
    group = planes * capacity
    stats = stats.reshape(2, columns, columns, group).transpose(2, 0, 1, 3)
    stats = stats.reshape(columns, 1, 2, OWN_ROWS)
    copies = jnp.broadcast_to(stats, (columns, lax.axis_size(VOC), 2, OWN_ROWS))
    copies = copies.reshape(-1, 2, OWN_ROWS)
    parts = lax.all_to_all(copies, PLANE, split_axis=0, concat_axis=0, tiled=True)
    row_top = jnp.max(parts[:, 0], axis=0)
    row_loss = row_top + jnp.log(jnp.sum(jnp.exp(parts[:, 0] - row_top[None]), axis=0))
    row_loss = row_loss - jnp.sum(parts[:, 1], axis=0)
    mine = row_labels.reshape(columns, columns, group)
    mine = lax.dynamic_index_in_dim(mine, here, axis=1, keepdims=False).reshape(-1)
    sent = jnp.where(mine >= 0, row_loss, 0.0).astype(jnp.float32)
    sent = sent.reshape(columns, planes, capacity).swapaxes(0, 1).reshape(planes, -1)
    return lax.all_to_all(sent, "z", split_axis=0, concat_axis=0, tiled=True).reshape(-1)


def solution(mesh):
    dp, vocab = mesh.shape["dp"], mesh.shape["vocab"]
    torus = Mesh(mesh.devices.reshape(dp // 4, 4, vocab // 2, 2), ("z", "x", "y", "c"))
    in_specs = (
        P(DP, None),
        P(DP, None, None),
        P(DP, None, None),
        P(DP, None, VOC),
        P(),
        P(VOC, DP),
    )
    return jax.shard_map(
        on_device, mesh=torus, in_specs=in_specs, out_specs=P(DP), check_vma=False
    )
```

```python
import functools

import jax
import jax.numpy as jnp
from jax import lax
from jax.experimental import pallas as pl
from jax.experimental.pallas import tpu as pltpu
from jax.sharding import Mesh
from jax.sharding import PartitionSpec as P


MAXSPAN = 5
OWN_ROWS = 768
DP = ("z", "x")
VOC = ("y", "c")
PLANE = ("x", "y", "c")


epsilon = 1e-06


ROW_BLOCK = 256
MATMUL_ROWS = 512
LANES = 128


def broadcast_all(value, axis):
    copies = jnp.broadcast_to(value, (lax.axis_size(axis), *value.shape))
    return lax.all_to_all(copies, axis, split_axis=0, concat_axis=0, tiled=True)


def swap_cores(value):
    return lax.ppermute(value, "c", [(0, 1), (1, 0)])


def part_width(rows, parts):
    return -(-rows // (parts * LANES)) * LANES


def exchanged_embedding(embedding):
    parts = lax.axis_size("x")
    local = embedding.T
    width, rows = local.shape
    part = part_width(rows, parts)
    local = jnp.pad(local, ((0, 0), (0, part * parts - rows)))
    split = jnp.stack([local[:, k * part : (k + 1) * part] for k in range(parts)])
    mixed = lax.all_to_all(split, "x", split_axis=0, concat_axis=0, tiled=True)
    return mixed.reshape(parts * width, part)


def packed_rows(tokens, span_bounds, owner, decoder_states):
    _, slot_count, local_width = decoder_states.shape
    planes, columns = lax.axis_size("z"), lax.axis_size("x")
    owner_total = planes * columns
    capacity = OWN_ROWS // owner_total
    slot_ids = jnp.arange(slot_count, dtype=jnp.int32)
    offsets = slot_ids % MAXSPAN
    starts = jnp.repeat(span_bounds[:, :, 0], MAXSPAN, axis=1)
    span_ends = jnp.repeat(span_bounds[:, :, 1], MAXSPAN, axis=1)
    is_live = (offsets[None, :] < span_ends - starts).reshape(-1)
    length = tokens.shape[1]
    positions = jnp.minimum(starts + offsets[None, :], length - 1)
    places = jnp.arange(length, dtype=jnp.int32)
    labels = jnp.sum(
        jnp.where(places[None, None, :] == positions[:, :, None], tokens[:, None, :], 0), axis=2
    ).reshape(-1)
    targets = owner.reshape(-1)
    slot_total = targets.shape[0]
    owner_hits = (targets[:, None] == jnp.arange(owner_total, dtype=jnp.int32)[None, :]).astype(
        jnp.bfloat16
    )
    device_slots = jnp.arange(slot_total, dtype=jnp.int32)
    earlier = (device_slots[:, None] > device_slots[None, :]).astype(jnp.bfloat16)
    running = jnp.dot(earlier, owner_hits, preferred_element_type=jnp.float32)
    slot_rank = jnp.sum(running * owner_hits.astype(jnp.float32), axis=1).astype(jnp.int32)
    place = (targets % columns) * planes + targets // columns
    target_row = place * capacity + slot_rank
    placing = (target_row[None, :] == jnp.arange(OWN_ROWS, dtype=jnp.int32)[:, None]) & is_live[
        None, :
    ]
    sent_labels = jnp.sum(jnp.where(placing, labels[None, :] + 1, 0), axis=1)
    onehot = placing.astype(jnp.bfloat16)
    states = decoder_states.reshape(slot_total, local_width)
    packed = jnp.dot(onehot, states, preferred_element_type=jnp.float32).astype(jnp.bfloat16)
    return packed, sent_labels


def normalize_block(core_ref, near_ref, far_ref, gain_ref, out_ref):
    first = core_ref[0] == 0
    pieces = []
    for k in range(near_ref.shape[1]):
        near = near_ref[0, k].astype(jnp.float32)
        far = far_ref[0, k].astype(jnp.float32)
        pieces += [jnp.where(first, near, far), jnp.where(first, far, near)]
    squares = pieces[0] * pieces[0]
    for piece in pieces[1:]:
        squares = squares + piece * piece
    width = len(pieces) * LANES
    mean_square = jnp.sum(squares, axis=1, keepdims=True) / width
    scale = lax.rsqrt(mean_square + epsilon)
    for k, piece in enumerate(pieces):
        gain = gain_ref[0:1, k * LANES : (k + 1) * LANES]
        out_ref[:, k * LANES : (k + 1) * LANES] = (
            piece * scale * gain * width ** (-0.5)
        ).astype(jnp.bfloat16)


def normalized(near, far, norm_gain):
    columns, slices = near.shape[:2]
    blocks = OWN_ROWS // ROW_BLOCK
    width = slices * 2 * LANES
    core = lax.axis_index("c").reshape(1)
    gain = norm_gain.astype(jnp.float32).reshape(1, width)
    spec = pl.BlockSpec((1, slices, ROW_BLOCK, LANES), lambda x, i, core: (x, 0, i, 0))
    return pl.pallas_call(
        normalize_block,
        grid_spec=pltpu.PrefetchScalarGridSpec(
            num_scalar_prefetch=1,
            grid=(columns, blocks),
            in_specs=[spec, spec, pl.BlockSpec((1, width), lambda x, i, core: (0, 0))],
            out_specs=pl.BlockSpec((ROW_BLOCK, width), lambda x, i, core: (x * blocks + i, 0)),
        ),
        out_shape=jax.ShapeDtypeStruct((columns * OWN_ROWS, width), jnp.bfloat16),
        name="normalized",
    )(core, near, far, gain)


def gathered_blocks(mixed):
    planes = lax.axis_size("z")

    def shifted(value, step):
        return lax.ppermute(value, "z", [(k, (k + step) % planes) for k in range(planes)])

    below = shifted(mixed, 5)
    above = shifted(mixed, -5)
    three = jnp.concatenate([mixed, below, above], axis=0)
    half = mixed.shape[0] // 2
    found = [(three, (0, -5, 5))]
    for step in (1, -1, 2, -2):
        found.append((shifted(three, step), (-step, -step - 5, -step + 5)))
    low = shifted(above[:half], -3)
    high = shifted(below[half:], 3)
    return found, (low, high)


def stats_block(scalars_ref, rows_ref, labels_ref, *refs, offsets):
    block_refs, (low_ref, high_ref, out_ref, weights_ref) = refs[: len(offsets)], refs[len(offsets) :]
    rows = rows_ref.shape[0]

    @pl.when(pl.program_id(0) == 0)
    def _():
        size = 2 * low_ref.shape[0]
        planes = weights_ref.shape[0] // size

        def place(offset):
            plane = (scalars_ref[1] + offset + planes) % planes
            return pl.multiple_of(plane * size, size)

        for ref, around in zip(block_refs, offsets):
            for k, offset in enumerate(around):
                weights_ref[pl.ds(place(offset), size), :] = ref[k * size : (k + 1) * size, :]
        middle = place(planes // 2)
        weights_ref[pl.ds(middle, size // 2), :] = low_ref[...]
        weights_ref[pl.ds(pl.multiple_of(middle + size // 2, size // 2), size // 2), :] = high_ref[...]

    logits = jnp.dot(rows_ref[...], weights_ref[...], preferred_element_type=jnp.float32)
    columns = lax.broadcasted_iota(jnp.int32, logits.shape, 1)
    logits = jnp.where(columns < scalars_ref[0], logits, -jnp.inf)
    top = jnp.max(logits, axis=1, keepdims=True)
    total = jnp.sum(jnp.exp(logits - top), axis=1, keepdims=True)
    label = jnp.broadcast_to(labels_ref[0:1, :], (LANES, rows)).T[:, 0:1]
    picked = jnp.sum(jnp.where(columns == label, logits, 0.0), axis=1, keepdims=True)
    lane = lax.broadcasted_iota(jnp.int32, (rows, LANES), 1)
    both = jnp.where(lane == 0, top + jnp.log(total), picked)
    out_ref[...] = both.T[0:8]


def row_stats(rows, blocks, labels, valid):
    total, width = rows.shape
    found, halves = blocks
    arrays = [array for array, _ in found] + list(halves)
    part = arrays[0].shape[1]
    scalars = jnp.stack([valid, lax.axis_index("z")]).astype(jnp.int32)
    whole = [pl.BlockSpec(array.shape, lambda i, scalars: (0, 0)) for array in arrays]
    stats = pl.pallas_call(
        functools.partial(stats_block, offsets=tuple(around for _, around in found)),
        grid_spec=pltpu.PrefetchScalarGridSpec(
            num_scalar_prefetch=1,
            grid=(total // MATMUL_ROWS,),
            in_specs=[
                pl.BlockSpec((MATMUL_ROWS, width), lambda i, scalars: (i, 0)),
                pl.BlockSpec((1, MATMUL_ROWS), lambda i, scalars: (0, i)),
                *whole,
            ],
            out_specs=pl.BlockSpec((8, MATMUL_ROWS), lambda i, scalars: (0, i)),
            scratch_shapes=[pltpu.VMEM((width, part), jnp.bfloat16)],
        ),
        out_shape=jax.ShapeDtypeStruct((8, total), jnp.float32),
        name="row_stats",
    )(scalars, rows, labels.reshape(1, total), *arrays)
    return stats[:2]


def on_device_body(tokens, span_bounds, owner, decoder_states, norm_gain, embedding):
    planes, columns = lax.axis_size("z"), lax.axis_size("x")
    capacity = OWN_ROWS // (planes * columns)
    shard_rows = embedding.shape[0]
    mixed = exchanged_embedding(embedding)
    mixed, tokens, span_bounds, owner, decoder_states = lax.optimization_barrier(
        (mixed, tokens, span_bounds, owner, decoder_states)
    )
    blocks = gathered_blocks(mixed)
    packed, sent_labels = packed_rows(tokens, span_bounds, owner, decoder_states)
    digits = jnp.stack([sent_labels // 256, sent_labels % 256]).astype(jnp.bfloat16)
    digits = digits.reshape(-1, LANES)
    digits = jnp.pad(digits, ((0, -digits.shape[0] % 16), (0, 0)))
    bundle = jnp.concatenate([packed, digits], axis=0)
    near = broadcast_all(bundle, ("x", "y"))
    far = swap_cores(near)
    near = near.reshape(columns, -1, *bundle.shape)
    far = far.reshape(near.shape)
    tags = near[:, 0, OWN_ROWS : OWN_ROWS + 2 * OWN_ROWS // LANES].astype(jnp.int32)
    tags = tags.reshape(columns, 2, OWN_ROWS)
    row_labels = tags[:, 0] * 256 + tags[:, 1] - 1
    part = mixed.shape[1]
    here = lax.axis_index("x")
    valid = jnp.minimum(shard_rows - here * part, part)
    local_label = row_labels - (lax.axis_index(VOC) * shard_rows + here * part)
    local_label = jnp.where((local_label >= 0) & (local_label < valid), local_label, -1)
    rows = normalized(near, far, norm_gain)
    stats = row_stats(rows, blocks, local_label.reshape(-1), valid)
    group = planes * capacity
    stats = stats.reshape(2, columns, columns, group).transpose(2, 0, 1, 3)
    stats = stats.reshape(columns, 1, 2, OWN_ROWS)
    copies = jnp.broadcast_to(stats, (columns, lax.axis_size(VOC), 2, OWN_ROWS))
    copies = copies.reshape(-1, 2, OWN_ROWS)
    parts = lax.all_to_all(copies, PLANE, split_axis=0, concat_axis=0, tiled=True)
    row_top = jnp.max(parts[:, 0], axis=0)
    row_loss = row_top + jnp.log(jnp.sum(jnp.exp(parts[:, 0] - row_top[None]), axis=0))
    row_loss = row_loss - jnp.sum(parts[:, 1], axis=0)
    mine = row_labels.reshape(columns, columns, group)
    mine = lax.dynamic_index_in_dim(mine, here, axis=1, keepdims=False).reshape(-1)
    sent = jnp.where(mine >= 0, row_loss, 0.0).astype(jnp.float32)
    sent = sent.reshape(columns, planes, capacity).swapaxes(0, 1).reshape(planes, -1)
    return lax.all_to_all(sent, "z", split_axis=0, concat_axis=0, tiled=True).reshape(-1)


def solution(mesh):
    dp, vocab = mesh.shape["dp"], mesh.shape["vocab"]
    torus = Mesh(mesh.devices.reshape(dp // 4, 4, vocab // 2, 2), ("z", "x", "y", "c"))
    in_specs = (
        P(DP, None),
        P(DP, None, None),
        P(DP, None, None),
        P(DP, None, VOC),
        P(),
        P(VOC, DP),
    )
    return jax.shard_map(
        on_device_body, mesh=torus, in_specs=in_specs, out_specs=P(DP), check_vma=False
    )
```

```python
import functools

import jax
import jax.numpy as jnp
from jax import lax
from jax.experimental import pallas as pl
from jax.experimental.pallas import tpu as pltpu
from jax.sharding import Mesh
from jax.sharding import PartitionSpec as P


MAXSPAN = 5
OWN_ROWS = 768
DP = ("z", "x")
VOC = ("y", "c")
PLANE = ("x", "y", "c")


epsilon = 1e-06


ROW_BLOCK = 256
HALF_ROWS = 384
CHUNK = 32
DEAD = -1e30
LANES = 128


def broadcast_all(value, axis):
    copies = jnp.broadcast_to(value, (lax.axis_size(axis), *value.shape))
    return lax.all_to_all(copies, axis, split_axis=0, concat_axis=0, tiled=True)


def swap_cores(value):
    return lax.ppermute(value, "c", [(0, 1), (1, 0)])


def part_width(rows, parts):
    return -(-rows // (parts * LANES)) * LANES


def exchanged_embedding(embedding):
    parts = lax.axis_size("x")
    local = embedding.T
    width, rows = local.shape
    part = part_width(rows, parts)
    local = jnp.pad(local, ((0, 0), (0, part * parts - rows)))
    split = jnp.stack([local[:, k * part : (k + 1) * part] for k in range(parts)])
    mixed = lax.all_to_all(split, "x", split_axis=0, concat_axis=0, tiled=True)
    return mixed.reshape(parts * width, part)


def packed_rows(tokens, span_bounds, owner, decoder_states):
    _, slot_count, local_width = decoder_states.shape
    planes, columns = lax.axis_size("z"), lax.axis_size("x")
    owner_total = planes * columns
    capacity = OWN_ROWS // owner_total
    slot_ids = jnp.arange(slot_count, dtype=jnp.int32)
    offsets = slot_ids % MAXSPAN
    starts = jnp.repeat(span_bounds[:, :, 0], MAXSPAN, axis=1)
    span_ends = jnp.repeat(span_bounds[:, :, 1], MAXSPAN, axis=1)
    is_live = (offsets[None, :] < span_ends - starts).reshape(-1)
    length = tokens.shape[1]
    positions = jnp.minimum(starts + offsets[None, :], length - 1)
    places = jnp.arange(length, dtype=jnp.int32)
    labels = jnp.sum(
        jnp.where(places[None, None, :] == positions[:, :, None], tokens[:, None, :], 0), axis=2
    ).reshape(-1)
    targets = owner.reshape(-1)
    slot_total = targets.shape[0]
    owner_hits = (targets[:, None] == jnp.arange(owner_total, dtype=jnp.int32)[None, :]).astype(
        jnp.bfloat16
    )
    device_slots = jnp.arange(slot_total, dtype=jnp.int32)
    earlier = (device_slots[:, None] > device_slots[None, :]).astype(jnp.bfloat16)
    running = jnp.dot(earlier, owner_hits, preferred_element_type=jnp.float32)
    slot_rank = jnp.sum(running * owner_hits.astype(jnp.float32), axis=1).astype(jnp.int32)
    target_row = targets * capacity + slot_rank
    placing = (target_row[None, :] == jnp.arange(OWN_ROWS, dtype=jnp.int32)[:, None]) & is_live[
        None, :
    ]
    sent_labels = jnp.sum(jnp.where(placing, labels[None, :] + 1, 0), axis=1)
    onehot = placing.astype(jnp.bfloat16)
    states = decoder_states.reshape(slot_total, local_width)
    packed = jnp.dot(onehot, states, preferred_element_type=jnp.float32).astype(jnp.bfloat16)
    return packed, sent_labels


def normalize_block(core_ref, near_ref, far_ref, gain_ref, out_ref):
    first = core_ref[0] == 0
    width = out_ref.shape[1]
    for start in range(0, out_ref.shape[0], CHUNK):
        pieces = []
        for k in range(near_ref.shape[1]):
            near = near_ref[0, k, start : start + CHUNK, :].astype(jnp.float32)
            far = far_ref[0, k, start : start + CHUNK, :].astype(jnp.float32)
            pieces += [jnp.where(first, near, far), jnp.where(first, far, near)]
        squares = pieces[0] * pieces[0]
        for piece in pieces[1:]:
            squares = squares + piece * piece
        mean_square = jnp.sum(squares, axis=1, keepdims=True) / width
        scale = lax.rsqrt(mean_square + epsilon)
        for k, piece in enumerate(pieces):
            gain = gain_ref[0:1, k * LANES : (k + 1) * LANES]
            out_ref[start : start + CHUNK, k * LANES : (k + 1) * LANES] = (
                piece * scale * gain
            ).astype(jnp.bfloat16)


def normalized(near, far, norm_gain):
    columns, slices = near.shape[:2]
    blocks = OWN_ROWS // ROW_BLOCK
    width = slices * 2 * LANES
    core = lax.axis_index("c").reshape(1)
    gain = (norm_gain.astype(jnp.float32) * width ** (-0.5)).reshape(1, width)
    spec = pl.BlockSpec((1, slices, ROW_BLOCK, LANES), lambda x, i, core: (x, 0, i, 0))
    return pl.pallas_call(
        normalize_block,
        grid_spec=pltpu.PrefetchScalarGridSpec(
            num_scalar_prefetch=1,
            grid=(columns, blocks),
            in_specs=[spec, spec, pl.BlockSpec((1, width), lambda x, i, core: (0, 0))],
            out_specs=pl.BlockSpec((ROW_BLOCK, width), lambda x, i, core: (x * blocks + i, 0)),
        ),
        out_shape=jax.ShapeDtypeStruct((columns * OWN_ROWS, width), jnp.bfloat16),
        name="normalized",
    )(core, near, far, gain)


def gathered_blocks(mixed):
    planes = lax.axis_size("z")

    def shifted(value, step):
        return lax.ppermute(value, "z", [(k, (k + step) % planes) for k in range(planes)])

    below = shifted(mixed, 5)
    above = shifted(mixed, -5)
    three, low, high = joined(mixed, below, above)
    found = [(three, (0, -5, 5))]
    for step in (1, -1, 2, -2):
        found.append((shifted(three, step), (-step, -step - 5, -step + 5)))
    low = shifted(low, -3)
    high = shifted(high, 3)
    return found, (low, high)


def joined_block(own_ref, below_ref, above_ref, three_ref, low_ref, high_ref):
    size = own_ref.shape[0]
    half = size // 2
    three_ref[0:size, :] = own_ref[...]
    three_ref[size : 2 * size, :] = below_ref[...]
    three_ref[2 * size : 3 * size, :] = above_ref[...]
    low_ref[...] = above_ref[0:half, :]
    high_ref[...] = below_ref[half:size, :]


def joined(own, below, above):
    size, part = own.shape
    return pl.pallas_call(
        joined_block,
        out_shape=tuple(
            jax.ShapeDtypeStruct((rows, part), own.dtype)
            for rows in (3 * size, size // 2, size // 2)
        ),
        name="joined",
    )(own, below, above)


def stats_block(scalars_ref, rows_ref, labels_ref, *refs, offsets):
    count = len(offsets)
    block_refs = refs[:count]
    low_ref, high_ref, out_ref, weights_ref, even_ref, odd_ref = refs[count:]
    step = pl.program_id(0)
    half = even_ref.shape[0]

    @pl.when(step == 0)
    def _():
        size = 2 * low_ref.shape[0]
        planes = weights_ref.shape[0] // size

        def place(offset):
            plane = (scalars_ref[1] + offset + planes) % planes
            return pl.multiple_of(plane * size, size)

        for ref, around in zip(block_refs, offsets):
            for k, offset in enumerate(around):
                weights_ref[pl.ds(place(offset), size), :] = ref[k * size : (k + 1) * size, :]
        middle = place(planes // 2)
        weights_ref[pl.ds(middle, size // 2), :] = low_ref[...]
        weights_ref[pl.ds(pl.multiple_of(middle + size // 2, size // 2), size // 2), :] = high_ref[...]

    def product(first):
        return jnp.dot(
            rows_ref[first : first + half, :], weights_ref[...], preferred_element_type=jnp.float32
        )

    def reduced(logits_ref, start):
        start = pl.multiple_of(start, LANES)
        part = logits_ref.shape[1]
        columns = lax.broadcasted_iota(jnp.int32, (CHUNK, part), 1)
        inside = columns < scalars_ref[0]
        lane = lax.broadcasted_iota(jnp.int32, (CHUNK, LANES), 1)
        for group in range(0, half, LANES):
            label_row = labels_ref[0:1, pl.ds(start + group, LANES)]
            label_all = jnp.broadcast_to(label_row, (LANES, LANES)).T
            pieces = []
            for chunk in range(0, LANES, CHUNK):
                label = label_all[chunk : chunk + CHUNK, 0:1]
                logits = logits_ref[group + chunk : group + chunk + CHUNK, :]
                logits = jnp.where(inside, logits, -jnp.inf)
                top = jnp.max(logits, axis=1, keepdims=True)
                total = jnp.sum(jnp.exp(logits - top), axis=1, keepdims=True)
                picked = jnp.sum(jnp.where(columns == label, logits, 0.0), axis=1, keepdims=True)
                value = jnp.where(label == -2, DEAD, top + jnp.log(total))
                pieces.append(jnp.where(lane == 0, value, picked))
            both = jnp.concatenate(pieces, axis=0).T
            out_ref[:, pl.ds(pl.multiple_of(start + group, LANES), LANES)] = both[0:8]

    total_rows = out_ref.shape[1]

    @pl.when(step < total_rows // (2 * half))
    def _():
        even_ref[...] = product(0)
        reduced(odd_ref, jnp.maximum(step * 2 - 1, 0) * half)
        odd_ref[...] = product(half)
        reduced(even_ref, step * 2 * half)

    @pl.when(step == total_rows // (2 * half))
    def _():
        reduced(odd_ref, total_rows - half)


def row_stats(rows, blocks, labels, valid):
    total, width = rows.shape
    found, halves = blocks
    arrays = [array for array, _ in found] + list(halves)
    part = arrays[0].shape[1]
    scalars = jnp.stack([valid, lax.axis_index("z")]).astype(jnp.int32)
    whole = [pl.BlockSpec(array.shape, lambda i, scalars: (0, 0)) for array in arrays]
    steps = total // (2 * HALF_ROWS)
    stats = pl.pallas_call(
        functools.partial(stats_block, offsets=tuple(around for _, around in found)),
        grid_spec=pltpu.PrefetchScalarGridSpec(
            num_scalar_prefetch=1,
            grid=(steps + 1,),
            in_specs=[
                pl.BlockSpec(
                    (2 * HALF_ROWS, width), lambda i, scalars: (jnp.minimum(i, steps - 1), 0)
                ),
                pl.BlockSpec((1, total), lambda i, scalars: (0, 0)),
                *whole,
            ],
            out_specs=pl.BlockSpec((8, total), lambda i, scalars: (0, 0)),
            scratch_shapes=[
                pltpu.VMEM((width, part), jnp.bfloat16),
                pltpu.VMEM((HALF_ROWS, part), jnp.float32),
                pltpu.VMEM((HALF_ROWS, part), jnp.float32),
            ],
        ),
        out_shape=jax.ShapeDtypeStruct((8, total), jnp.float32),
        name="row_stats",
    )(scalars, rows, labels.reshape(1, total), *arrays)
    return stats[:2]


def on_device_body(tokens, span_bounds, owner, decoder_states, norm_gain, embedding):
    planes, columns = lax.axis_size("z"), lax.axis_size("x")
    capacity = OWN_ROWS // (planes * columns)
    shard_rows = embedding.shape[0]
    mixed = exchanged_embedding(embedding)
    blocks = gathered_blocks(mixed)
    packed, sent_labels = packed_rows(tokens, span_bounds, owner, decoder_states)
    digits = jnp.stack([sent_labels // 256, sent_labels % 256]).astype(jnp.bfloat16)
    digits = digits.reshape(-1, LANES)
    digits = jnp.pad(digits, ((0, -digits.shape[0] % 16), (0, 0)))
    bundle = jnp.concatenate([packed, digits], axis=0)
    near = broadcast_all(bundle, ("x", "y"))
    far = swap_cores(near)
    near = near.reshape(columns, -1, *bundle.shape)
    far = far.reshape(near.shape)
    tags = near[:, 0, OWN_ROWS : OWN_ROWS + 2 * OWN_ROWS // LANES].astype(jnp.int32)
    tags = tags.reshape(columns, 2, OWN_ROWS)
    row_labels = tags[:, 0] * 256 + tags[:, 1] - 1
    part = mixed.shape[1]
    here = lax.axis_index("x")
    valid = jnp.minimum(shard_rows - here * part, part)
    local_label = row_labels - (lax.axis_index(VOC) * shard_rows + here * part)
    local_label = jnp.where((local_label >= 0) & (local_label < valid), local_label, -1)
    local_label = jnp.where(row_labels < 0, -2, local_label)
    rows = normalized(near, far, norm_gain)
    stats = row_stats(rows, blocks, local_label.reshape(-1), valid)
    share = 2 * columns * capacity
    owners = planes * columns
    stats = stats.reshape(2 * columns, owners, capacity).swapaxes(0, 1).reshape(owners, 1, share)
    copies = jnp.broadcast_to(stats, (owners, lax.axis_size(VOC), share)).reshape(-1, share)
    parts = lax.all_to_all(copies, ("z", *PLANE), split_axis=0, concat_axis=0, tiled=True)
    parts = parts.reshape(planes, -1, share)
    values, picked = parts[:, :, : share // 2], parts[:, :, share // 2 :]
    row_top = jnp.max(values, axis=1)
    row_loss = row_top + jnp.log(jnp.sum(jnp.exp(values - row_top[:, None]), axis=1))
    row_loss = row_loss - jnp.sum(picked, axis=1)
    return jnp.where(row_top > 0.5 * DEAD, row_loss, 0.0).reshape(-1).astype(jnp.float32)


def solution(mesh):
    dp, vocab = mesh.shape["dp"], mesh.shape["vocab"]
    torus = Mesh(mesh.devices.reshape(dp // 4, 4, vocab // 2, 2), ("z", "x", "y", "c"))
    in_specs = (
        P(DP, None),
        P(DP, None, None),
        P(DP, None, None),
        P(DP, None, VOC),
        P(),
        P(VOC, DP),
    )
    return jax.shard_map(
        on_device_body, mesh=torus, in_specs=in_specs, out_specs=P(DP), check_vma=False
    )
```

```python
import functools

import jax
import jax.numpy as jnp
from jax import lax
from jax.experimental import pallas as pl
from jax.experimental.pallas import tpu as pltpu
from jax.sharding import Mesh
from jax.sharding import PartitionSpec as P


MAXSPAN = 5
OWN_ROWS = 768
DP = ("z", "x")
VOC = ("y", "c")
PLANE = ("x", "y", "c")


epsilon = 1e-06


ROW_BLOCK = 384
LANES = 128


def broadcast_all(value, axis):
    copies = jnp.broadcast_to(value, (lax.axis_size(axis), *value.shape))
    return lax.all_to_all(copies, axis, split_axis=0, concat_axis=0, tiled=True)


def swap_cores(value):
    return lax.ppermute(value, "c", [(0, 1), (1, 0)])


def part_width(rows, parts):
    return -(-rows // (parts * LANES)) * LANES


def exchanged_embedding(embedding):
    parts = lax.axis_size("x")
    local = embedding.T
    width, rows = local.shape
    part = part_width(rows, parts)
    local = jnp.pad(local, ((0, 0), (0, part * parts - rows)))
    split = jnp.stack([local[:, k * part : (k + 1) * part] for k in range(parts)])
    mixed = lax.all_to_all(split, "x", split_axis=0, concat_axis=0, tiled=True)
    return mixed.reshape(parts * width, part)


def packed_rows(tokens, span_bounds, owner, decoder_states):
    _, slot_count, local_width = decoder_states.shape
    planes, columns = lax.axis_size("z"), lax.axis_size("x")
    owner_total = planes * columns
    capacity = OWN_ROWS // owner_total
    slot_ids = jnp.arange(slot_count, dtype=jnp.int32)
    offsets = slot_ids % MAXSPAN
    starts = jnp.repeat(span_bounds[:, :, 0], MAXSPAN, axis=1)
    span_ends = jnp.repeat(span_bounds[:, :, 1], MAXSPAN, axis=1)
    is_live = (offsets[None, :] < span_ends - starts).reshape(-1)
    length = tokens.shape[1]
    positions = jnp.minimum(starts + offsets[None, :], length - 1)
    places = jnp.arange(length, dtype=jnp.int32)
    labels = jnp.sum(
        jnp.where(places[None, None, :] == positions[:, :, None], tokens[:, None, :], 0), axis=2
    ).reshape(-1)
    targets = owner.reshape(-1)
    slot_total = targets.shape[0]
    owner_hits = (targets[:, None] == jnp.arange(owner_total, dtype=jnp.int32)[None, :]).astype(
        jnp.bfloat16
    )
    device_slots = jnp.arange(slot_total, dtype=jnp.int32)
    earlier = (device_slots[:, None] > device_slots[None, :]).astype(jnp.bfloat16)
    running = jnp.dot(earlier, owner_hits, preferred_element_type=jnp.float32)
    slot_rank = jnp.sum(running * owner_hits.astype(jnp.float32), axis=1).astype(jnp.int32)
    target_row = targets * capacity + slot_rank
    placing = (target_row[None, :] == jnp.arange(OWN_ROWS, dtype=jnp.int32)[:, None]) & is_live[
        None, :
    ]
    sent_labels = jnp.sum(jnp.where(placing, labels[None, :] + 1, 0), axis=1)
    onehot = placing.astype(jnp.bfloat16)
    states = decoder_states.reshape(slot_total, local_width)
    packed = jnp.dot(onehot, states, preferred_element_type=jnp.float32).astype(jnp.bfloat16)
    return packed, sent_labels


def gathered_blocks(mixed):
    planes = lax.axis_size("z")

    def shifted(value, step):
        return lax.ppermute(value, "z", [(k, (k + step) % planes) for k in range(planes)])

    below = shifted(mixed, 5)
    above = shifted(mixed, -5)
    three, low, high = joined(mixed, below, above)
    found = [(three, (0, -5, 5))]
    for step in (1, -1, 2, -2):
        found.append((shifted(three, step), (-step, -step - 5, -step + 5)))
    low = shifted(low, -3)
    high = shifted(high, 3)
    return found, (low, high)


def joined_block(own_ref, below_ref, above_ref, three_ref, low_ref, high_ref):
    size = own_ref.shape[0]
    half = size // 2
    three_ref[0:size, :] = own_ref[...]
    three_ref[size : 2 * size, :] = below_ref[...]
    three_ref[2 * size : 3 * size, :] = above_ref[...]
    low_ref[...] = above_ref[0:half, :]
    high_ref[...] = below_ref[half:size, :]


def joined(own, below, above):
    size, part = own.shape
    return pl.pallas_call(
        joined_block,
        out_shape=tuple(
            jax.ShapeDtypeStruct((rows, part), own.dtype)
            for rows in (3 * size, size // 2, size // 2)
        ),
        name="joined",
    )(own, below, above)


def stats_block(scalars_ref, near_ref, far_ref, gain_ref, labels_ref, *refs, offsets):
    count = len(offsets)
    block_refs, (low_ref, high_ref, out_ref, weights_ref) = refs[:count], refs[count:]
    rows, width = near_ref.shape[2], weights_ref.shape[0]
    part = weights_ref.shape[1]

    @pl.when((pl.program_id(0) == 0) & (pl.program_id(1) == 0))
    def _():
        size = 2 * low_ref.shape[0]
        planes = width // size

        def place(offset):
            plane = (scalars_ref[1] + offset + planes) % planes
            return pl.multiple_of(plane * size, size)

        for ref, around in zip(block_refs, offsets):
            for k, offset in enumerate(around):
                weights_ref[pl.ds(place(offset), size), :] = ref[k * size : (k + 1) * size, :]
        middle = place(planes // 2)
        weights_ref[pl.ds(middle, size // 2), :] = low_ref[...]
        middle = pl.multiple_of(middle + size // 2, size // 2)
        weights_ref[pl.ds(middle, size // 2), :] = high_ref[...]

    north = scalars_ref[2] == 0
    pieces = []
    for k in range(near_ref.shape[1]):
        near = near_ref[0, k].astype(jnp.float32)
        far = far_ref[0, k].astype(jnp.float32)
        pieces += [jnp.where(north, near, far), jnp.where(north, far, near)]
    squares = pieces[0] * pieces[0]
    for piece in pieces[1:]:
        squares = squares + piece * piece
    mean_square = jnp.sum(squares, axis=1, keepdims=True) / width
    scale = lax.rsqrt(mean_square + epsilon)
    normed = jnp.concatenate(
        [
            (piece * scale * gain_ref[0:1, k * LANES : (k + 1) * LANES]).astype(jnp.bfloat16)
            for k, piece in enumerate(pieces)
        ],
        axis=1,
    )
    logits = jnp.dot(normed, weights_ref[...], preferred_element_type=jnp.float32)
    columns = lax.broadcasted_iota(jnp.int32, (rows, part), 1)
    logits = jnp.where(columns < scalars_ref[0], logits, -jnp.inf)
    top = jnp.max(logits, axis=1, keepdims=True)
    total = jnp.sum(jnp.exp(logits - top), axis=1, keepdims=True)
    label = jnp.broadcast_to(labels_ref[0:1, :], (LANES, rows)).T[:, 0:1]
    picked = jnp.sum(jnp.where(columns == label, logits, 0.0), axis=1, keepdims=True)
    lane = lax.broadcasted_iota(jnp.int32, (rows, LANES), 1)
    both = jnp.where(lane == 0, top + jnp.log(total), picked)
    out_ref[...] = both.T[0:8]


def row_stats(near, far, gain, blocks, labels, valid):
    sources, slices = near.shape[:2]
    steps = OWN_ROWS // ROW_BLOCK
    width = slices * 2 * LANES
    found, halves = blocks
    arrays = [array for array, _ in found] + list(halves)
    part = arrays[0].shape[1]
    plane, core = lax.axis_index("z"), lax.axis_index("c")
    scalars = jnp.stack([valid, plane, core]).astype(jnp.int32)
    rows = pl.BlockSpec((1, slices, ROW_BLOCK, LANES), lambda x, i, scalars: (x, 0, i, 0))
    whole = [
        pl.BlockSpec(array.shape, lambda x, i, scalars: (0, 0)) for array in (gain, *arrays)
    ]
    stats = pl.pallas_call(
        functools.partial(stats_block, offsets=tuple(around for _, around in found)),
        grid_spec=pltpu.PrefetchScalarGridSpec(
            num_scalar_prefetch=1,
            grid=(sources, steps),
            in_specs=[
                rows,
                rows,
                whole[0],
                pl.BlockSpec((1, ROW_BLOCK), lambda x, i, scalars: (0, x * steps + i)),
                *whole[1:],
            ],
            out_specs=pl.BlockSpec((8, ROW_BLOCK), lambda x, i, scalars: (0, x * steps + i)),
            scratch_shapes=[pltpu.VMEM((width, part), jnp.bfloat16)],
        ),
        out_shape=jax.ShapeDtypeStruct((8, sources * OWN_ROWS), jnp.float32),
        name="row_stats",
    )(scalars, near, far, gain, labels.reshape(1, -1), *arrays)
    return stats[:2]


def on_device_body(tokens, span_bounds, owner, decoder_states, norm_gain, embedding):
    planes, columns = lax.axis_size("z"), lax.axis_size("x")
    capacity = OWN_ROWS // (planes * columns)
    shard_rows = embedding.shape[0]
    mixed = exchanged_embedding(embedding)
    blocks = gathered_blocks(mixed)
    packed, sent_labels = packed_rows(tokens, span_bounds, owner, decoder_states)
    group = columns * capacity
    width = packed.shape[1]
    digits = jnp.stack([sent_labels // 256, sent_labels % 256]).astype(jnp.bfloat16)
    digits = digits.reshape(2, planes, group).swapaxes(0, 1)
    digits = jnp.pad(digits, ((0, 0), (0, 6), (0, width - group)))
    sent = jnp.concatenate([packed.reshape(planes, group, width), digits], axis=1)
    arrived = lax.all_to_all(sent, "z", split_axis=0, concat_axis=0, tiled=True)
    bundle = jnp.concatenate(
        [
            arrived[:, :group].reshape(OWN_ROWS, width),
            arrived[:, group],
            arrived[:, group + 1],
        ],
        axis=0,
    )
    near = broadcast_all(bundle, ("x", "y"))
    far = swap_cores(near)
    near = near.reshape(columns, -1, *bundle.shape)
    far = far.reshape(near.shape)
    tags = near[:, 0, OWN_ROWS : OWN_ROWS + 2 * planes].astype(jnp.int32)
    tags = tags.reshape(columns, 2, planes, width)[..., :group]
    row_labels = tags[:, 0] * 256 + tags[:, 1] - 1
    part = mixed.shape[1]
    here = lax.axis_index("x")
    valid = jnp.minimum(shard_rows - here * part, part)
    local_label = row_labels - (lax.axis_index(VOC) * shard_rows + here * part)
    local_label = jnp.where((local_label >= 0) & (local_label < valid), local_label, -1)
    gain = (norm_gain.astype(jnp.float32) * norm_gain.shape[0] ** (-0.5)).reshape(1, -1)
    stats = row_stats(near, far, gain, blocks, local_label.reshape(-1), valid)
    stats = stats.reshape(2, columns, planes, columns, capacity).transpose(3, 0, 2, 1, 4)
    stats = stats.reshape(columns, 1, 2, OWN_ROWS)
    copies = jnp.broadcast_to(stats, (columns, lax.axis_size(VOC), 2, OWN_ROWS))
    copies = copies.reshape(-1, 2, OWN_ROWS)
    parts = lax.all_to_all(copies, PLANE, split_axis=0, concat_axis=0, tiled=True)
    row_top = jnp.max(parts[:, 0], axis=0)
    row_loss = row_top + jnp.log(jnp.sum(jnp.exp(parts[:, 0] - row_top[None]), axis=0))
    row_loss = row_loss - jnp.sum(parts[:, 1], axis=0)
    mine = row_labels.reshape(columns, planes, columns, capacity)
    mine = lax.dynamic_index_in_dim(mine, here, axis=2, keepdims=False)
    live = mine.swapaxes(0, 1).reshape(-1) >= 0
    return jnp.where(live, row_loss, 0.0).astype(jnp.float32)


def solution(mesh):
    dp, vocab = mesh.shape["dp"], mesh.shape["vocab"]
    torus = Mesh(mesh.devices.reshape(dp // 4, 4, vocab // 2, 2), ("z", "x", "y", "c"))
    in_specs = (
        P(DP, None),
        P(DP, None, None),
        P(DP, None, None),
        P(DP, None, VOC),
        P(),
        P(VOC, DP),
    )
    return jax.shard_map(
        on_device_body, mesh=torus, in_specs=in_specs, out_specs=P(DP), check_vma=False
    )
```

```python
import functools

import jax
import jax.numpy as jnp
from jax import lax
from jax.experimental import pallas as pl
from jax.experimental.pallas import tpu as pltpu
from jax.sharding import Mesh
from jax.sharding import PartitionSpec as P


MAXSPAN = 5
OWN_ROWS = 768
DP = ("z", "x")
VOC = ("y", "c")
PLANE = ("x", "y", "c")


epsilon = 1e-06


GROUP = 128
LANES = 128


def broadcast_all(value, axis):
    copies = jnp.broadcast_to(value, (lax.axis_size(axis), *value.shape))
    return lax.all_to_all(copies, axis, split_axis=0, concat_axis=0, tiled=True)


def swap_cores(value):
    return lax.ppermute(value, "c", [(0, 1), (1, 0)])


def part_width(rows, parts):
    return -(-rows // (parts * LANES)) * LANES


def exchanged_embedding(embedding):
    parts = lax.axis_size("x")
    local = embedding.T
    width, rows = local.shape
    part = part_width(rows, parts)
    local = jnp.pad(local, ((0, 0), (0, part * parts - rows)))
    split = jnp.stack([local[:, k * part : (k + 1) * part] for k in range(parts)])
    mixed = lax.all_to_all(split, "x", split_axis=0, concat_axis=0, tiled=True)
    return mixed.reshape(parts * width, part)


def packed_rows(tokens, span_bounds, owner, decoder_states):
    _, slot_count, local_width = decoder_states.shape
    planes, columns = lax.axis_size("z"), lax.axis_size("x")
    owner_total = planes * columns
    capacity = OWN_ROWS // owner_total
    slot_ids = jnp.arange(slot_count, dtype=jnp.int32)
    offsets = slot_ids % MAXSPAN
    starts = jnp.repeat(span_bounds[:, :, 0], MAXSPAN, axis=1)
    span_ends = jnp.repeat(span_bounds[:, :, 1], MAXSPAN, axis=1)
    is_live = (offsets[None, :] < span_ends - starts).reshape(-1)
    length = tokens.shape[1]
    positions = jnp.minimum(starts + offsets[None, :], length - 1)
    places = jnp.arange(length, dtype=jnp.int32)
    labels = jnp.sum(
        jnp.where(places[None, None, :] == positions[:, :, None], tokens[:, None, :], 0), axis=2
    ).reshape(-1)
    targets = owner.reshape(-1)
    slot_total = targets.shape[0]
    owner_hits = (targets[:, None] == jnp.arange(owner_total, dtype=jnp.int32)[None, :]).astype(
        jnp.bfloat16
    )
    device_slots = jnp.arange(slot_total, dtype=jnp.int32)
    earlier = (device_slots[:, None] > device_slots[None, :]).astype(jnp.bfloat16)
    running = jnp.dot(earlier, owner_hits, preferred_element_type=jnp.float32)
    slot_rank = jnp.sum(running * owner_hits.astype(jnp.float32), axis=1).astype(jnp.int32)
    target_row = targets * capacity + slot_rank
    placing = (target_row[None, :] == jnp.arange(OWN_ROWS, dtype=jnp.int32)[:, None]) & is_live[
        None, :
    ]
    sent_labels = jnp.sum(jnp.where(placing, labels[None, :] + 1, 0), axis=1)
    onehot = placing.astype(jnp.bfloat16)
    states = decoder_states.reshape(slot_total, local_width)
    packed = jnp.dot(onehot, states, preferred_element_type=jnp.float32).astype(jnp.bfloat16)
    return packed, sent_labels


def gathered_blocks(mixed):
    planes = lax.axis_size("z")

    def shifted(value, step):
        return lax.ppermute(value, "z", [(k, (k + step) % planes) for k in range(planes)])

    below = shifted(mixed, 5)
    above = shifted(mixed, -5)
    three, low, high = joined(mixed, below, above)
    found = [(three, (0, -5, 5))]
    for step in (1, -1, 2, -2):
        found.append((shifted(three, step), (-step, -step - 5, -step + 5)))
    low = shifted(low, -3)
    high = shifted(high, 3)
    return found, (low, high)


def joined_block(own_ref, below_ref, above_ref, three_ref, low_ref, high_ref):
    size = own_ref.shape[0]
    half = size // 2
    three_ref[0:size, :] = own_ref[...]
    three_ref[size : 2 * size, :] = below_ref[...]
    three_ref[2 * size : 3 * size, :] = above_ref[...]
    low_ref[...] = above_ref[0:half, :]
    high_ref[...] = below_ref[half:size, :]


def joined(own, below, above):
    size, part = own.shape
    return pl.pallas_call(
        joined_block,
        out_shape=tuple(
            jax.ShapeDtypeStruct((rows, part), own.dtype)
            for rows in (3 * size, size // 2, size // 2)
        ),
        name="joined",
    )(own, below, above)


def stats_block(scalars_ref, near_ref, far_ref, gain_ref, labels_ref, *refs, offsets):
    count = len(offsets)
    block_refs = refs[:count]
    low_ref, high_ref, out_ref, weights_ref, even_ref, odd_ref = refs[count:]
    rows, width = even_ref.shape[0], weights_ref.shape[0]
    part = weights_ref.shape[1]

    @pl.when(pl.program_id(0) == 0)
    def _():
        size = 2 * low_ref.shape[0]
        planes = width // size

        def place(offset):
            plane = (scalars_ref[1] + offset + planes) % planes
            return pl.multiple_of(plane * size, size)

        for ref, around in zip(block_refs, offsets):
            for k, offset in enumerate(around):
                weights_ref[pl.ds(place(offset), size), :] = ref[k * size : (k + 1) * size, :]
        middle = place(planes // 2)
        weights_ref[pl.ds(middle, size // 2), :] = low_ref[...]
        middle = pl.multiple_of(middle + size // 2, size // 2)
        weights_ref[pl.ds(middle, size // 2), :] = high_ref[...]

    def normed(first):
        north = scalars_ref[2] == 0
        pieces = []
        for k in range(near_ref.shape[1]):
            near = near_ref[0, k, first : first + rows, :].astype(jnp.float32)
            far = far_ref[0, k, first : first + rows, :].astype(jnp.float32)
            pieces += [jnp.where(north, near, far), jnp.where(north, far, near)]
        squares = pieces[0] * pieces[0]
        for piece in pieces[1:]:
            squares = squares + piece * piece
        mean_square = jnp.sum(squares, axis=1, keepdims=True) / width
        scale = lax.rsqrt(mean_square + epsilon)
        return jnp.concatenate(
            [
                (piece * scale * gain_ref[0:1, k * LANES : (k + 1) * LANES]).astype(jnp.bfloat16)
                for k, piece in enumerate(pieces)
            ],
            axis=1,
        )

    def product(values):
        return jnp.dot(values, weights_ref[...], preferred_element_type=jnp.float32)

    def reduced(logits_ref, start):
        for group in range(0, rows, GROUP):
            place = pl.ds(pl.multiple_of(start + group, LANES), GROUP)
            lane = lax.broadcasted_iota(jnp.int32, (GROUP, LANES), 1)
            tiles = [
                logits_ref[group : group + GROUP, first : first + LANES]
                for first in range(0, part, LANES)
            ]
            tiles[-1] = jnp.where(lane < scalars_ref[0] - (part - LANES), tiles[-1], -jnp.inf)
            top = functools.reduce(jnp.maximum, tiles)
            top = jnp.max(top, axis=1, keepdims=True)
            total = functools.reduce(jnp.add, [jnp.exp(tile - top) for tile in tiles])
            total = jnp.sum(total, axis=1, keepdims=True)
            label = jnp.broadcast_to(labels_ref[0:1, place], (LANES, GROUP)).T
            ahead = label - lane
            picked = jnp.zeros((GROUP, LANES), jnp.float32)
            for k, tile in enumerate(tiles):
                picked = jnp.where(ahead == k * LANES, tile, picked)
            picked = jnp.sum(picked, axis=1, keepdims=True)
            both = jnp.where(lane == 0, top + jnp.log(total), picked)
            out_ref[:, place] = both.T[0:2]

    step = pl.program_id(0)
    last = pl.num_programs(0) - 1

    @pl.when(step < last)
    def _():
        even_ref[...] = product(normed(0))
        reduced(odd_ref, jnp.maximum(2 * step - 1, 0) * rows)
        odd_ref[...] = product(normed(rows))
        reduced(even_ref, 2 * step * rows)

    @pl.when(step == last)
    def _():
        reduced(odd_ref, (2 * last - 1) * rows)


def row_stats(near, far, gain, blocks, labels, valid):
    sources, slices = near.shape[:2]
    width = slices * 2 * LANES
    found, halves = blocks
    arrays = [array for array, _ in found] + list(halves)
    part = arrays[0].shape[1]
    plane, core = lax.axis_index("z"), lax.axis_index("c")
    scalars = jnp.stack([valid, plane, core]).astype(jnp.int32)
    rows = pl.BlockSpec(
        (1, slices, OWN_ROWS, LANES), lambda x, scalars: (jnp.minimum(x, sources - 1), 0, 0, 0)
    )
    whole = [
        pl.BlockSpec(array.shape, lambda x, scalars: (0, 0)) for array in (gain, *arrays)
    ]
    return pl.pallas_call(
        functools.partial(stats_block, offsets=tuple(around for _, around in found)),
        grid_spec=pltpu.PrefetchScalarGridSpec(
            num_scalar_prefetch=1,
            grid=(sources + 1,),
            in_specs=[
                rows,
                rows,
                whole[0],
                pl.BlockSpec((1, sources * OWN_ROWS), lambda x, scalars: (0, 0)),
                *whole[1:],
            ],
            out_specs=pl.BlockSpec((2, sources * OWN_ROWS), lambda x, scalars: (0, 0)),
            scratch_shapes=[
                pltpu.VMEM((width, part), jnp.bfloat16),
                pltpu.VMEM((OWN_ROWS // 2, part), jnp.float32),
                pltpu.VMEM((OWN_ROWS // 2, part), jnp.float32),
            ],
        ),
        out_shape=jax.ShapeDtypeStruct((2, sources * OWN_ROWS), jnp.float32),
        name="row_stats",
    )(scalars, near, far, gain, labels.reshape(1, -1), *arrays)


def on_device_body(tokens, span_bounds, owner, decoder_states, norm_gain, embedding):
    planes, columns = lax.axis_size("z"), lax.axis_size("x")
    capacity = OWN_ROWS // (planes * columns)
    shard_rows = embedding.shape[0]
    mixed = exchanged_embedding(embedding)
    blocks = gathered_blocks(mixed)
    packed, sent_labels = packed_rows(tokens, span_bounds, owner, decoder_states)
    group = columns * capacity
    width = packed.shape[1]
    digits = jnp.stack([sent_labels // 256, sent_labels % 256]).astype(jnp.bfloat16)
    digits = digits.reshape(2, planes, group).swapaxes(0, 1)
    digits = jnp.pad(digits, ((0, 0), (0, 6), (0, width - group)))
    sent = jnp.concatenate([packed.reshape(planes, group, width), digits], axis=1)
    arrived = lax.all_to_all(sent, "z", split_axis=0, concat_axis=0, tiled=True)
    bundle = jnp.concatenate(
        [
            arrived[:, :group].reshape(OWN_ROWS, width),
            arrived[:, group],
            arrived[:, group + 1],
        ],
        axis=0,
    )
    near = broadcast_all(bundle, ("x", "y"))
    far = swap_cores(near)
    near = near.reshape(columns, -1, *bundle.shape)
    far = far.reshape(near.shape)
    tags = near[:, 0, OWN_ROWS : OWN_ROWS + 2 * planes].astype(jnp.int32)
    tags = tags.reshape(columns, 2, planes, width)[..., :group]
    row_labels = tags[:, 0] * 256 + tags[:, 1] - 1
    part = mixed.shape[1]
    assert columns * part - shard_rows < LANES
    here = lax.axis_index("x")
    valid = jnp.minimum(shard_rows - here * part, part)
    local_label = row_labels - (lax.axis_index(VOC) * shard_rows + here * part)
    local_label = jnp.where((local_label >= 0) & (local_label < valid), local_label, -1)
    gain = (norm_gain.astype(jnp.float32) * norm_gain.shape[0] ** (-0.5)).reshape(1, -1)
    stats = row_stats(near, far, gain, blocks, local_label.reshape(-1), valid)
    stats = stats.reshape(2, columns, planes, columns, capacity).transpose(3, 0, 2, 1, 4)
    stats = stats.reshape(columns, 1, 2, OWN_ROWS)
    copies = jnp.broadcast_to(stats, (columns, lax.axis_size(VOC), 2, OWN_ROWS))
    copies = copies.reshape(-1, 2, OWN_ROWS)
    parts = lax.all_to_all(copies, PLANE, split_axis=0, concat_axis=0, tiled=True)
    row_top = jnp.max(parts[:, 0], axis=0)
    row_loss = row_top + jnp.log(jnp.sum(jnp.exp(parts[:, 0] - row_top[None]), axis=0))
    row_loss = row_loss - jnp.sum(parts[:, 1], axis=0)
    mine = row_labels.reshape(columns, planes, columns, capacity)
    mine = lax.dynamic_index_in_dim(mine, here, axis=2, keepdims=False)
    live = mine.swapaxes(0, 1).reshape(-1) >= 0
    return jnp.where(live, row_loss, 0.0).astype(jnp.float32)


def solution(mesh):
    dp, vocab = mesh.shape["dp"], mesh.shape["vocab"]
    torus = Mesh(mesh.devices.reshape(dp // 4, 4, vocab // 2, 2), ("z", "x", "y", "c"))
    in_specs = (
        P(DP, None),
        P(DP, None, None),
        P(DP, None, None),
        P(DP, None, VOC),
        P(),
        P(VOC, DP),
    )
    return jax.shard_map(
        on_device_body, mesh=torus, in_specs=in_specs, out_specs=P(DP), check_vma=False
    )
```

```python
import functools

import jax
import jax.numpy as jnp
from jax import lax
from jax.experimental import pallas as pl
from jax.experimental.pallas import tpu as pltpu
from jax.sharding import Mesh
from jax.sharding import PartitionSpec as P


MAXSPAN = 5
OWN_ROWS = 768
DP = ("z", "x")
VOC = ("y", "c")
PLANE = ("x", "y", "c")


epsilon = 1e-06


GROUP = 128
LANES = 128


def spread_block(arrived_ref, tags_ref, out_ref, *, group):
    planes = arrived_ref.shape[0]
    for k in range(planes):
        out_ref[0, k * group : (k + 1) * group, :] = arrived_ref[k, 0:group, :]
    out_ref[0, planes * group : planes * group + planes, :] = tags_ref[...]


def spread(arrived, tags, group, copies):
    planes, _, width = arrived.shape
    rows = planes * (group + 1)
    return pl.pallas_call(
        functools.partial(spread_block, group=group),
        grid=(copies,),
        in_specs=[
            pl.BlockSpec(arrived.shape, lambda i: (0, 0, 0)),
            pl.BlockSpec(tags.shape, lambda i: (0, 0)),
        ],
        out_specs=pl.BlockSpec((1, rows, width), lambda i: (i, 0, 0)),
        out_shape=jax.ShapeDtypeStruct((copies, rows, width), arrived.dtype),
        name="spread",
    )(arrived, tags)


def swap_cores(value):
    return lax.ppermute(value, "c", [(0, 1), (1, 0)])


def part_width(rows, parts):
    return -(-rows // (parts * LANES)) * LANES


def exchanged_embedding(embedding):
    parts = lax.axis_size("x")
    local = embedding.T
    width, rows = local.shape
    part = part_width(rows, parts)
    local = jnp.pad(local, ((0, 0), (0, part * parts - rows)))
    split = jnp.stack([local[:, k * part : (k + 1) * part] for k in range(parts)])
    mixed = lax.all_to_all(split, "x", split_axis=0, concat_axis=0, tiled=True)
    return mixed.reshape(parts * width, part)


def packed_rows(tokens, span_bounds, owner, decoder_states):
    _, slot_count, local_width = decoder_states.shape
    planes, columns = lax.axis_size("z"), lax.axis_size("x")
    owner_total = planes * columns
    capacity = OWN_ROWS // owner_total
    slot_ids = jnp.arange(slot_count, dtype=jnp.int32)
    offsets = slot_ids % MAXSPAN
    starts = jnp.repeat(span_bounds[:, :, 0], MAXSPAN, axis=1)
    span_ends = jnp.repeat(span_bounds[:, :, 1], MAXSPAN, axis=1)
    is_live = (offsets[None, :] < span_ends - starts).reshape(-1)
    length = tokens.shape[1]
    positions = jnp.minimum(starts + offsets[None, :], length - 1)
    places = jnp.arange(length, dtype=jnp.int32)
    labels = jnp.sum(
        jnp.where(places[None, None, :] == positions[:, :, None], tokens[:, None, :], 0), axis=2
    ).reshape(-1)
    targets = owner.reshape(-1)
    slot_total = targets.shape[0]
    owner_hits = (targets[:, None] == jnp.arange(owner_total, dtype=jnp.int32)[None, :]).astype(
        jnp.bfloat16
    )
    device_slots = jnp.arange(slot_total, dtype=jnp.int32)
    earlier = (device_slots[:, None] > device_slots[None, :]).astype(jnp.bfloat16)
    running = jnp.dot(earlier, owner_hits, preferred_element_type=jnp.float32)
    slot_rank = jnp.sum(running * owner_hits.astype(jnp.float32), axis=1).astype(jnp.int32)
    target_row = targets * capacity + slot_rank
    placing = (target_row[None, :] == jnp.arange(OWN_ROWS, dtype=jnp.int32)[:, None]) & is_live[
        None, :
    ]
    sent_labels = jnp.sum(jnp.where(placing, labels[None, :] + 1, 0), axis=1)
    onehot = placing.astype(jnp.bfloat16)
    states = decoder_states.reshape(slot_total, local_width)
    packed = jnp.dot(onehot, states, preferred_element_type=jnp.float32).astype(jnp.bfloat16)
    return packed, sent_labels


def gathered_blocks(mixed):
    planes = lax.axis_size("z")

    def shifted(value, step):
        return lax.ppermute(value, "z", [(k, (k + step) % planes) for k in range(planes)])

    below = shifted(mixed, 5)
    above = shifted(mixed, -5)
    three, low, high = joined(mixed, below, above)
    found = [(three, (0, -5, 5))]
    for step in (1, -1, 2, -2):
        found.append((shifted(three, step), (-step, -step - 5, -step + 5)))
    low = shifted(low, -3)
    high = shifted(high, 3)
    return found, (low, high)


def joined_block(own_ref, below_ref, above_ref, three_ref, low_ref, high_ref):
    size = own_ref.shape[0]
    half = size // 2
    three_ref[0:size, :] = own_ref[...]
    three_ref[size : 2 * size, :] = below_ref[...]
    three_ref[2 * size : 3 * size, :] = above_ref[...]
    low_ref[...] = above_ref[0:half, :]
    high_ref[...] = below_ref[half:size, :]


def joined(own, below, above):
    size, part = own.shape
    return pl.pallas_call(
        joined_block,
        out_shape=tuple(
            jax.ShapeDtypeStruct((rows, part), own.dtype)
            for rows in (3 * size, size // 2, size // 2)
        ),
        name="joined",
    )(own, below, above)


def stats_block(scalars_ref, near_ref, far_ref, gain_ref, labels_ref, *refs, offsets):
    count = len(offsets)
    block_refs = refs[:count]
    low_ref, high_ref, out_ref, weights_ref, even_ref, odd_ref = refs[count:]
    rows, width = even_ref.shape[0], weights_ref.shape[0]
    part = weights_ref.shape[1]

    @pl.when(pl.program_id(0) == 0)
    def _():
        size = 2 * low_ref.shape[0]
        planes = width // size

        def place(offset):
            plane = (scalars_ref[1] + offset + planes) % planes
            return pl.multiple_of(plane * size, size)

        for ref, around in zip(block_refs, offsets):
            for k, offset in enumerate(around):
                weights_ref[pl.ds(place(offset), size), :] = ref[k * size : (k + 1) * size, :]
        middle = place(planes // 2)
        weights_ref[pl.ds(middle, size // 2), :] = low_ref[...]
        middle = pl.multiple_of(middle + size // 2, size // 2)
        weights_ref[pl.ds(middle, size // 2), :] = high_ref[...]

    def normed(first):
        north = scalars_ref[2] == 0
        pieces = []
        for k in range(near_ref.shape[1]):
            near = near_ref[0, k, first : first + rows, :].astype(jnp.float32)
            far = far_ref[0, k, first : first + rows, :].astype(jnp.float32)
            pieces += [jnp.where(north, near, far), jnp.where(north, far, near)]
        squares = pieces[0] * pieces[0]
        for piece in pieces[1:]:
            squares = squares + piece * piece
        mean_square = jnp.sum(squares, axis=1, keepdims=True) / width
        scale = lax.rsqrt(mean_square + epsilon)
        return jnp.concatenate(
            [
                (piece * scale * gain_ref[0:1, k * LANES : (k + 1) * LANES]).astype(jnp.bfloat16)
                for k, piece in enumerate(pieces)
            ],
            axis=1,
        )

    def product(values):
        return jnp.dot(values, weights_ref[...], preferred_element_type=jnp.float32)

    def reduced(logits_ref, start):
        for group in range(0, rows, GROUP):
            place = pl.ds(pl.multiple_of(start + group, LANES), GROUP)
            lane = lax.broadcasted_iota(jnp.int32, (GROUP, LANES), 1)
            tiles = [
                logits_ref[group : group + GROUP, first : first + LANES]
                for first in range(0, part, LANES)
            ]
            tiles[-1] = jnp.where(lane < scalars_ref[0] - (part - LANES), tiles[-1], -jnp.inf)
            top = functools.reduce(jnp.maximum, tiles)
            top = jnp.max(top, axis=1, keepdims=True)
            total = functools.reduce(jnp.add, [jnp.exp(tile - top) for tile in tiles])
            total = jnp.sum(total, axis=1, keepdims=True)
            label = jnp.broadcast_to(labels_ref[0:1, place], (LANES, GROUP)).T
            ahead = label - lane
            picked = jnp.zeros((GROUP, LANES), jnp.float32)
            for k, tile in enumerate(tiles):
                picked = jnp.where(ahead == k * LANES, tile, picked)
            picked = jnp.sum(picked, axis=1, keepdims=True)
            both = jnp.where(lane == 0, top + jnp.log(total), picked)
            out_ref[:, place] = both.T[0:2]

    step = pl.program_id(0)
    last = pl.num_programs(0) - 1

    @pl.when(step < last)
    def _():
        even_ref[...] = product(normed(0))
        reduced(odd_ref, jnp.maximum(2 * step - 1, 0) * rows)
        odd_ref[...] = product(normed(rows))
        reduced(even_ref, 2 * step * rows)

    @pl.when(step == last)
    def _():
        reduced(odd_ref, (2 * last - 1) * rows)


def row_stats(near, far, gain, blocks, labels, valid):
    sources, slices = near.shape[:2]
    width = slices * 2 * LANES
    found, halves = blocks
    arrays = [array for array, _ in found] + list(halves)
    part = arrays[0].shape[1]
    plane, core = lax.axis_index("z"), lax.axis_index("c")
    scalars = jnp.stack([valid, plane, core]).astype(jnp.int32)
    rows = pl.BlockSpec(
        (1, slices, OWN_ROWS, LANES), lambda x, scalars: (jnp.minimum(x, sources - 1), 0, 0, 0)
    )
    whole = [
        pl.BlockSpec(array.shape, lambda x, scalars: (0, 0)) for array in (gain, *arrays)
    ]
    return pl.pallas_call(
        functools.partial(stats_block, offsets=tuple(around for _, around in found)),
        grid_spec=pltpu.PrefetchScalarGridSpec(
            num_scalar_prefetch=1,
            grid=(sources + 1,),
            in_specs=[
                rows,
                rows,
                whole[0],
                pl.BlockSpec((1, sources * OWN_ROWS), lambda x, scalars: (0, 0)),
                *whole[1:],
            ],
            out_specs=pl.BlockSpec((2, sources * OWN_ROWS), lambda x, scalars: (0, 0)),
            scratch_shapes=[
                pltpu.VMEM((width, part), jnp.bfloat16),
                pltpu.VMEM((OWN_ROWS // 2, part), jnp.float32),
                pltpu.VMEM((OWN_ROWS // 2, part), jnp.float32),
            ],
        ),
        out_shape=jax.ShapeDtypeStruct((2, sources * OWN_ROWS), jnp.float32),
        name="row_stats",
    )(scalars, near, far, gain, labels.reshape(1, -1), *arrays)


def on_device_body(tokens, span_bounds, owner, decoder_states, norm_gain, embedding):
    planes, columns = lax.axis_size("z"), lax.axis_size("x")
    capacity = OWN_ROWS // (planes * columns)
    shard_rows = embedding.shape[0]
    mixed = exchanged_embedding(embedding)
    blocks = gathered_blocks(mixed)
    packed, sent_labels = packed_rows(tokens, span_bounds, owner, decoder_states)
    group = columns * capacity
    width = packed.shape[1]
    digits = jnp.stack([sent_labels // 256, sent_labels % 256]).astype(jnp.bfloat16)
    digits = digits.reshape(2, planes, group).swapaxes(0, 1).reshape(planes, 1, 2 * group)
    digits = jnp.pad(digits, ((0, 0), (0, 7), (0, width - 2 * group)))
    sent = jnp.concatenate([packed.reshape(planes, group, width), digits], axis=1)
    arrived = lax.all_to_all(sent, "z", split_axis=0, concat_axis=0, tiled=True)
    copies = spread(arrived, arrived[:, group], group, lax.axis_size(("x", "y")))
    near = lax.all_to_all(copies, ("x", "y"), split_axis=0, concat_axis=0, tiled=True)
    far = swap_cores(near)
    near = near.reshape(columns, -1, *near.shape[1:])
    far = far.reshape(near.shape)
    tags = near[:, 0, OWN_ROWS : OWN_ROWS + planes].astype(jnp.int32)
    row_labels = tags[..., :group] * 256 + tags[..., group : 2 * group] - 1
    part = mixed.shape[1]
    assert columns * part - shard_rows < LANES
    here = lax.axis_index("x")
    valid = jnp.minimum(shard_rows - here * part, part)
    local_label = row_labels - (lax.axis_index(VOC) * shard_rows + here * part)
    local_label = jnp.where((local_label >= 0) & (local_label < valid), local_label, -1)
    gain = (norm_gain.astype(jnp.float32) * norm_gain.shape[0] ** (-0.5)).reshape(1, -1)
    stats = row_stats(near, far, gain, blocks, local_label.reshape(-1), valid)
    stats = stats.reshape(2, columns, planes, columns, capacity).transpose(3, 0, 2, 1, 4)
    stats = stats.reshape(columns, 1, 2, OWN_ROWS)
    copies = jnp.broadcast_to(stats, (columns, lax.axis_size(VOC), 2, OWN_ROWS))
    copies = copies.reshape(-1, 2, OWN_ROWS)
    parts = lax.all_to_all(copies, PLANE, split_axis=0, concat_axis=0, tiled=True)
    row_top = jnp.max(parts[:, 0], axis=0)
    row_loss = row_top + jnp.log(jnp.sum(jnp.exp(parts[:, 0] - row_top[None]), axis=0))
    row_loss = row_loss - jnp.sum(parts[:, 1], axis=0)
    mine = row_labels.reshape(columns, planes, columns, capacity)
    mine = lax.dynamic_index_in_dim(mine, here, axis=2, keepdims=False)
    live = mine.swapaxes(0, 1).reshape(-1) >= 0
    return jnp.where(live, row_loss, 0.0).astype(jnp.float32)


def solution(mesh):
    dp, vocab = mesh.shape["dp"], mesh.shape["vocab"]
    torus = Mesh(mesh.devices.reshape(dp // 4, 4, vocab // 2, 2), ("z", "x", "y", "c"))
    in_specs = (
        P(DP, None),
        P(DP, None, None),
        P(DP, None, None),
        P(DP, None, VOC),
        P(),
        P(VOC, DP),
    )
    return jax.shard_map(
        on_device_body, mesh=torus, in_specs=in_specs, out_specs=P(DP), check_vma=False
    )
```

```python
import functools

import jax
import jax.numpy as jnp
from jax import lax
from jax.experimental import pallas as pl
from jax.experimental.pallas import tpu as pltpu
from jax.sharding import Mesh
from jax.sharding import PartitionSpec as P


MAXSPAN = 5
OWN_ROWS = 768
DP = ("z", "x")
VOC = ("y", "c")
PLANE = ("x", "y", "c")


epsilon = 1e-06


GROUP = 128
LANES = 128


def broadcast_all(value, axis):
    copies = jnp.broadcast_to(value, (lax.axis_size(axis), *value.shape))
    return lax.all_to_all(copies, axis, split_axis=0, concat_axis=0, tiled=True)


def swap_cores(value):
    return lax.ppermute(value, "c", [(0, 1), (1, 0)])


def part_width(rows, parts):
    return -(-rows // (parts * LANES)) * LANES


def exchanged_embedding(embedding):
    parts = lax.axis_size("x")
    local = embedding.T
    width, rows = local.shape
    part = part_width(rows, parts)
    local = jnp.pad(local, ((0, 0), (0, part * parts - rows)))
    split = jnp.stack([local[:, k * part : (k + 1) * part] for k in range(parts)])
    mixed = lax.all_to_all(split, "x", split_axis=0, concat_axis=0, tiled=True)
    return mixed.reshape(parts * width, part)


def packed_rows(tokens, span_bounds, owner, decoder_states):
    _, slot_count, local_width = decoder_states.shape
    planes, columns = lax.axis_size("z"), lax.axis_size("x")
    owner_total = planes * columns
    capacity = OWN_ROWS // owner_total
    slot_ids = jnp.arange(slot_count, dtype=jnp.int32)
    offsets = slot_ids % MAXSPAN
    starts = jnp.repeat(span_bounds[:, :, 0], MAXSPAN, axis=1)
    span_ends = jnp.repeat(span_bounds[:, :, 1], MAXSPAN, axis=1)
    is_live = (offsets[None, :] < span_ends - starts).reshape(-1)
    length = tokens.shape[1]
    positions = jnp.minimum(starts + offsets[None, :], length - 1)
    places = jnp.arange(length, dtype=jnp.int32)
    labels = jnp.sum(
        jnp.where(places[None, None, :] == positions[:, :, None], tokens[:, None, :], 0), axis=2
    ).reshape(-1)
    targets = owner.reshape(-1)
    slot_total = targets.shape[0]
    owner_hits = (targets[:, None] == jnp.arange(owner_total, dtype=jnp.int32)[None, :]).astype(
        jnp.bfloat16
    )
    device_slots = jnp.arange(slot_total, dtype=jnp.int32)
    earlier = (device_slots[:, None] > device_slots[None, :]).astype(jnp.bfloat16)
    running = jnp.dot(earlier, owner_hits, preferred_element_type=jnp.float32)
    slot_rank = jnp.sum(running * owner_hits.astype(jnp.float32), axis=1).astype(jnp.int32)
    target_row = targets * capacity + slot_rank
    placing = (target_row[None, :] == jnp.arange(OWN_ROWS, dtype=jnp.int32)[:, None]) & is_live[
        None, :
    ]
    sent_labels = jnp.sum(jnp.where(placing, labels[None, :] + 1, 0), axis=1)
    onehot = placing.astype(jnp.bfloat16)
    states = decoder_states.reshape(slot_total, local_width)
    packed = jnp.dot(onehot, states, preferred_element_type=jnp.float32).astype(jnp.bfloat16)
    return packed, sent_labels


def gathered_blocks(mixed):
    planes = lax.axis_size("z")

    def shifted(value, step):
        return lax.ppermute(value, "z", [(k, (k + step) % planes) for k in range(planes)])

    below = shifted(mixed, 5)
    above = shifted(mixed, -5)
    three, low, high = joined(mixed, below, above)
    found = [(three, (0, -5, 5))]
    for step in (1, -1, 2, -2):
        found.append((shifted(three, step), (-step, -step - 5, -step + 5)))
    low = shifted(low, -3)
    high = shifted(high, 3)
    return found, (low, high)


def joined_block(own_ref, below_ref, above_ref, three_ref, low_ref, high_ref):
    size = own_ref.shape[0]
    half = size // 2
    three_ref[0:size, :] = own_ref[...]
    three_ref[size : 2 * size, :] = below_ref[...]
    three_ref[2 * size : 3 * size, :] = above_ref[...]
    low_ref[...] = above_ref[0:half, :]
    high_ref[...] = below_ref[half:size, :]


def joined(own, below, above):
    size, part = own.shape
    return pl.pallas_call(
        joined_block,
        out_shape=tuple(
            jax.ShapeDtypeStruct((rows, part), own.dtype)
            for rows in (3 * size, size // 2, size // 2)
        ),
        name="joined",
    )(own, below, above)


def stats_block(scalars_ref, near_ref, far_ref, gain_ref, labels_ref, *refs, offsets):
    count = len(offsets)
    block_refs = refs[:count]
    low_ref, high_ref, out_ref, weights_ref, even_ref, odd_ref = refs[count:]
    rows, width = even_ref.shape[0], weights_ref.shape[0]
    part = weights_ref.shape[1]

    @pl.when(pl.program_id(0) == 0)
    def _():
        size = 2 * low_ref.shape[0]
        planes = width // size

        def place(offset):
            plane = (scalars_ref[1] + offset + planes) % planes
            return pl.multiple_of(plane * size, size)

        for ref, around in zip(block_refs, offsets):
            for k, offset in enumerate(around):
                weights_ref[pl.ds(place(offset), size), :] = ref[k * size : (k + 1) * size, :]
        middle = place(planes // 2)
        weights_ref[pl.ds(middle, size // 2), :] = low_ref[...]
        middle = pl.multiple_of(middle + size // 2, size // 2)
        weights_ref[pl.ds(middle, size // 2), :] = high_ref[...]

    def normed(first):
        north = scalars_ref[2] == 0
        pieces = []
        for k in range(near_ref.shape[1]):
            near = near_ref[0, k, first : first + rows, :].astype(jnp.float32)
            far = far_ref[0, k, first : first + rows, :].astype(jnp.float32)
            pieces += [jnp.where(north, near, far), jnp.where(north, far, near)]
        squares = pieces[0] * pieces[0]
        for piece in pieces[1:]:
            squares = squares + piece * piece
        mean_square = jnp.sum(squares, axis=1, keepdims=True) / width
        scale = lax.rsqrt(mean_square + epsilon)
        return jnp.concatenate(
            [
                (piece * scale * gain_ref[0:1, k * LANES : (k + 1) * LANES]).astype(jnp.bfloat16)
                for k, piece in enumerate(pieces)
            ],
            axis=1,
        )

    def product(values):
        return jnp.dot(values, weights_ref[...], preferred_element_type=jnp.float32)

    def reduced(logits_ref, start):
        for group in range(0, rows, GROUP):
            place = pl.ds(pl.multiple_of(start + group, LANES), GROUP)
            lane = lax.broadcasted_iota(jnp.int32, (GROUP, LANES), 1)
            tiles = [
                logits_ref[group : group + GROUP, first : first + LANES]
                for first in range(0, part, LANES)
            ]
            tiles[-1] = jnp.where(lane < scalars_ref[0] - (part - LANES), tiles[-1], -jnp.inf)
            top = functools.reduce(jnp.maximum, tiles)
            top = jnp.max(top, axis=1, keepdims=True)
            total = functools.reduce(jnp.add, [jnp.exp(tile - top) for tile in tiles])
            total = jnp.sum(total, axis=1, keepdims=True)
            label = jnp.broadcast_to(labels_ref[0:1, place], (LANES, GROUP)).T
            ahead = label - lane
            picked = jnp.zeros((GROUP, LANES), jnp.float32)
            for k, tile in enumerate(tiles):
                picked = jnp.where(ahead == k * LANES, tile, picked)
            picked = jnp.sum(picked, axis=1, keepdims=True)
            both = jnp.where(lane == 0, top + jnp.log(total), picked)
            out_ref[:, place] = both.T[0:2]

    step = pl.program_id(0)
    last = pl.num_programs(0) - 1

    @pl.when(step < last)
    def _():
        even_ref[...] = product(normed(0))
        reduced(odd_ref, jnp.maximum(2 * step - 1, 0) * rows)
        odd_ref[...] = product(normed(rows))
        reduced(even_ref, 2 * step * rows)

    @pl.when(step == last)
    def _():
        reduced(odd_ref, (2 * last - 1) * rows)


def row_stats(near, far, gain, blocks, labels, valid):
    sources, slices = near.shape[:2]
    width = slices * 2 * LANES
    found, halves = blocks
    arrays = [array for array, _ in found] + list(halves)
    part = arrays[0].shape[1]
    plane, core = lax.axis_index("z"), lax.axis_index("c")
    scalars = jnp.stack([valid, plane, core]).astype(jnp.int32)
    rows = pl.BlockSpec(
        (1, slices, OWN_ROWS, LANES), lambda x, scalars: (jnp.minimum(x, sources - 1), 0, 0, 0)
    )
    whole = [
        pl.BlockSpec(array.shape, lambda x, scalars: (0, 0)) for array in (gain, *arrays)
    ]
    return pl.pallas_call(
        functools.partial(stats_block, offsets=tuple(around for _, around in found)),
        grid_spec=pltpu.PrefetchScalarGridSpec(
            num_scalar_prefetch=1,
            grid=(sources + 1,),
            in_specs=[
                rows,
                rows,
                whole[0],
                pl.BlockSpec((1, sources * OWN_ROWS), lambda x, scalars: (0, 0)),
                *whole[1:],
            ],
            out_specs=pl.BlockSpec((2, sources * OWN_ROWS), lambda x, scalars: (0, 0)),
            scratch_shapes=[
                pltpu.VMEM((width, part), jnp.bfloat16),
                pltpu.VMEM((OWN_ROWS // 2, part), jnp.float32),
                pltpu.VMEM((OWN_ROWS // 2, part), jnp.float32),
            ],
        ),
        out_shape=jax.ShapeDtypeStruct((2, sources * OWN_ROWS), jnp.float32),
        name="row_stats",
    )(scalars, near, far, gain, labels.reshape(1, -1), *arrays)


def on_device_body(tokens, span_bounds, owner, decoder_states, norm_gain, embedding):
    planes, columns = lax.axis_size("z"), lax.axis_size("x")
    capacity = OWN_ROWS // (planes * columns)
    shard_rows = embedding.shape[0]
    mixed = exchanged_embedding(embedding)
    blocks = gathered_blocks(mixed)
    packed, sent_labels = packed_rows(tokens, span_bounds, owner, decoder_states)
    group = columns * capacity
    width = packed.shape[1]
    digits = jnp.stack([sent_labels // 256, sent_labels % 256]).astype(jnp.bfloat16)
    digits = digits.reshape(2, planes, group).swapaxes(0, 1).reshape(planes, 1, 2 * group)
    digits = jnp.pad(digits, ((0, 0), (0, 7), (0, width - 2 * group)))
    sent = jnp.concatenate([packed.reshape(planes, group, width), digits], axis=1)
    arrived = lax.all_to_all(sent, "z", split_axis=0, concat_axis=0, tiled=True)
    bundle = jnp.concatenate(
        [
            arrived[:, :group].reshape(OWN_ROWS, width),
            arrived[:, group],
        ],
        axis=0,
    )
    near = broadcast_all(bundle, ("x", "y"))
    far = swap_cores(near)
    near = near.reshape(columns, -1, *bundle.shape)
    far = far.reshape(near.shape)
    tags = near[:, 0, OWN_ROWS : OWN_ROWS + planes].astype(jnp.int32)
    row_labels = tags[..., :group] * 256 + tags[..., group : 2 * group] - 1
    part = mixed.shape[1]
    assert columns * part - shard_rows < LANES
    here = lax.axis_index("x")
    valid = jnp.minimum(shard_rows - here * part, part)
    local_label = row_labels - (lax.axis_index(VOC) * shard_rows + here * part)
    local_label = jnp.where((local_label >= 0) & (local_label < valid), local_label, -1)
    gain = (norm_gain.astype(jnp.float32) * norm_gain.shape[0] ** (-0.5)).reshape(1, -1)
    stats = row_stats(near, far, gain, blocks, local_label.reshape(-1), valid)
    stats = stats.reshape(2, columns, planes, columns, capacity).transpose(3, 0, 2, 1, 4)
    stats = stats.reshape(columns, 1, 2, OWN_ROWS)
    copies = jnp.broadcast_to(stats, (columns, lax.axis_size(VOC), 2, OWN_ROWS))
    copies = copies.reshape(-1, 2, OWN_ROWS)
    parts = lax.all_to_all(copies, PLANE, split_axis=0, concat_axis=0, tiled=True)
    row_top = jnp.max(parts[:, 0], axis=0)
    row_loss = row_top + jnp.log(jnp.sum(jnp.exp(parts[:, 0] - row_top[None]), axis=0))
    row_loss = row_loss - jnp.sum(parts[:, 1], axis=0)
    mine = row_labels.reshape(columns, planes, columns, capacity)
    mine = lax.dynamic_index_in_dim(mine, here, axis=2, keepdims=False)
    live = mine.swapaxes(0, 1).reshape(-1) >= 0
    return jnp.where(live, row_loss, 0.0).astype(jnp.float32)


def solution(mesh):
    dp, vocab = mesh.shape["dp"], mesh.shape["vocab"]
    torus = Mesh(mesh.devices.reshape(dp // 4, 4, vocab // 2, 2), ("z", "x", "y", "c"))
    in_specs = (
        P(DP, None),
        P(DP, None, None),
        P(DP, None, None),
        P(DP, None, VOC),
        P(),
        P(VOC, DP),
    )
    return jax.shard_map(
        on_device_body, mesh=torus, in_specs=in_specs, out_specs=P(DP), check_vma=False
    )
```
